512 devices in a mesh: gx: 8 (over x, core), gy: 8 (over z_lo), gz: 8 (over z_hi, y).
Axes of the slice: x: 4, y: 4, z: 16 (z_hi: 2, z_lo: 8; z = z_hi * 8 + z_lo), core: 2. Of those that a mesh axis runs over, the one named last changes fastest.
Arguments:
- attn_out: bfloat16 [1408, 8192], P('gx', ('gz', 'gy')), may hold values from -6 to 6
- residual: bfloat16 [1408, 8192], P('gx', ('gy', 'gz')), may hold values from -60 to 60
- proj_weight: bfloat16 [8192, 8192], P(('gz', 'gx'), 'gy'), may hold values from -0.0625 to 0.0625
- norm_gain: float32 [8192], P(('gy', 'gz')), may hold values from 0.1 to 1.9
- gate_proj: bfloat16 [8192, 14336], P(('gy', 'gx'), 'gz'), may hold values from -0.0625 to 0.0625
- up_proj: bfloat16 [8192, 14336], P(('gy', 'gx'), 'gz'), may hold values from -0.0625 to 0.0625
- down_proj: bfloat16 [14336, 8192], P(('gz', 'gx'), 'gy'), may hold values from -0.046875 to 0.046875
Outputs:
- layer_out: bfloat16 [1408, 8192], P('gx', ('gy', 'gz'))
The draws below stay inside these ranges and needn't reach their ends.
All inputs are finite; a program needn't handle non-finite values.
Results may differ from the reference program's by a relative error of at most 0.0029.
Values may be sent and summed in bfloat16 or wider, within the bound.
No kernel may reach another device: no remote copies, remote signals or barrier semaphores. Data moves between devices by JAX's collectives and lax.ppermute only.
A program may use at most 64 MiB of HBM per device.

```python
import jax
import jax.numpy as jnp
from jax import lax

D = 8192
FFW = 14336
TOKENS = 1408


def draw_residual(key, part):
    first, second = jax.random.split(key, 2)
    ramp = 1.0 + 2.0 * jnp.arange(D, dtype=jnp.float32)[None, :] / (D - 1)
    values = jnp.clip(jax.random.normal(first, (TOKENS, D), jnp.float32), -6.0, 6.0)
    scales = jnp.exp(jax.random.uniform(second, (TOKENS, 1), jnp.float32, jnp.log(0.3), jnp.log(3.0)))
    return (values * scales * ramp).astype(jnp.bfloat16)


def block_scale(rng, shape, shards, smallest, high):
    loudness, own = 1.0, jax.random.fold_in(rng, 6)
    for dim, parts in shards:
        steps = jnp.exp(jax.random.uniform(jax.random.fold_in(own, dim), (parts,), jnp.float32, smallest / len(shards), high / len(shards)))
        loudness = loudness * jnp.repeat(steps, shape[dim] // parts).reshape([-1 if axis == dim else 1 for axis in range(len(shape))])
    return loudness


def centred(rng, extent, scale, reach, cuts=(), held_as=jnp.bfloat16):
    factor_of = block_scale(rng, extent, cuts, -0.22, 0.18) if cuts else 1.0
    result = jax.random.normal(rng, extent, jnp.float32) * scale * factor_of
    return jnp.minimum(jnp.maximum(result, -reach), reach).astype(held_as)


def setup_inputs(seed: int = 0) -> dict:
    key_of = jax.random.split(jax.random.key(seed), 8)
    return {
        "attn_out": centred(key_of[0], (TOKENS, D), 1.0, 6.0, ((0, 8), (1, 64))),
        "residual": draw_residual(jax.random.fold_in(key_of[7], 71), 0),
        "proj_weight": centred(key_of[2], (D, D), D ** -0.5, 0.0625, ((0, 64), (1, 8))),
        "norm_gain": jnp.clip(1.0 + 0.18 * jax.random.normal(key_of[3], (D,), jnp.float32), 0.1, 1.9),
        "gate_proj": centred(key_of[4], (D, FFW), D ** -0.5, 0.0625, ((0, 64), (1, 8))),
        "up_proj": centred(key_of[5], (D, FFW), D ** -0.5, 0.0625, ((0, 64), (1, 8))),
        "down_proj": centred(key_of[6], (FFW, D), FFW ** -0.5, 0.046875, ((0, 64), (1, 8))),
    }


def reference(attn_out, residual, proj_weight, norm_gain, gate_proj, up_proj, down_proj):
    projected = jnp.dot(attn_out, proj_weight, preferred_element_type=jnp.float32)
    stream = residual.astype(jnp.float32) + projected
    inverse = lax.rsqrt(lax.optimization_barrier(jnp.mean(stream * stream, axis=1, keepdims=True)) + 1e-05)
    scaled = (stream * norm_gain.astype(jnp.float32)[None, :]).astype(jnp.bfloat16)
    gate_sum = inverse * jnp.dot(scaled, gate_proj, preferred_element_type=jnp.float32)
    up_sum = inverse * jnp.dot(scaled, up_proj, preferred_element_type=jnp.float32)
    hidden = (jax.nn.silu(gate_sum) * up_sum).astype(jnp.bfloat16)
    down_sum = jnp.dot(hidden, down_proj, preferred_element_type=jnp.float32)
    return (stream + down_sum).astype(jnp.bfloat16)
```

```python
import jax
import jax.numpy as jnp
from jax import lax
from jax.sharding import Mesh
from jax.sharding import PartitionSpec as P

D = 8192
BF = jnp.bfloat16
F32 = jnp.float32
AXES = ("x", "c", "zl", "zh", "y")


def shift(value, axis, step):
    n = lax.axis_size(axis)
    return lax.ppermute(value, axis, [(i, (i + step) % n) for i in range(n)])


def swap(value, axis, bit=1):
    n = lax.axis_size(axis)
    return lax.ppermute(value, axis, [(i, i ^ bit) for i in range(n)])


def pick(value, index, dim=0):
    return lax.dynamic_index_in_dim(value, index, dim, keepdims=False)


def from_everyone(value, axis):
    copies = jnp.broadcast_to(value, (lax.axis_size(axis), *value.shape))
    return lax.all_to_all(copies, axis, split_axis=0, concat_axis=0, tiled=True)


def in_bits(own, other, bit):
    first = jnp.where(bit == 0, own, other)
    second = jnp.where(bit == 0, other, own)
    return first, second


def ring_shards(w):
    return [w, shift(w, "x", 1), shift(w, "x", 2), shift(w, "x", -1)]


def dot(a, b):
    return jnp.dot(a, b, preferred_element_type=F32)


def relative(blocks, xi, core):
    parts = [pick(pick(blocks, (xi - k) % 4), core) for k in range(4)]
    return jnp.concatenate(parts, axis=1)


def sums_over_y(part):
    blocks = part.astype(BF).reshape(-1, 2, 4, 128).transpose(2, 1, 0, 3)
    arrived = lax.all_to_all(blocks, "y", split_axis=0, concat_axis=0, tiled=True)
    return arrived.astype(F32).sum(axis=0)


def exact(value):
    return lax.reduce_precision(value, 8, 7)


def on_device(attn_out, residual, proj_weight, norm_gain, gate_proj, up_proj, down_proj):
    xi, ci = lax.axis_index("x"), lax.axis_index("c")
    zl, zh = lax.axis_index("zl"), lax.axis_index("zh")
    bit0, bit1, bit2 = zl & 1, (zl >> 1) & 1, (zl >> 2) & 1
    rows = attn_out.shape[0]
    half = rows // 2
    top = 48
    step = half - top
    ffw = gate_proj.shape[1] // 2

    proj_own = jnp.concatenate(ring_shards(proj_weight))
    proj_other = swap(proj_own, "c")
    cols = from_everyone(attn_out, "zl").reshape(4, 2, rows, 128)

    high = exact(norm_gain)
    mid = exact(norm_gain - high)
    low = norm_gain - high - mid
    gains = jnp.stack([high, mid, low]).astype(BF)
    facing = swap(jnp.concatenate([residual, jnp.pad(gains, ((0, 5), (0, 0)))]), "zh")
    other_gain = facing[rows : rows + 3].astype(F32).sum(axis=0)
    residual2 = jnp.stack(in_bits(residual, facing[:rows], zh)).astype(F32)
    gain2 = jnp.stack(in_bits(norm_gain, other_gain, zh))

    pieces = [gate_proj[:, :ffw], up_proj[:, :ffw], gate_proj[:, ffw:], up_proj[:, ffw:]]
    both_own = jnp.concatenate(ring_shards(jnp.concatenate(pieces, axis=1)))
    both_other = swap(both_own, "c")
    down_own = jnp.concatenate(ring_shards(down_proj))
    down_other = swap(down_own, "c")
    height = down_proj.shape[0]
    down_all = jnp.zeros((4, 2, height, down_proj.shape[1]), BF)
    for k in range(4):
        at = (xi - k) % 4
        mine = down_own[k * height : (k + 1) * height][None, None]
        theirs = down_other[k * height : (k + 1) * height][None, None]
        down_all = lax.dynamic_update_slice(down_all, mine, (at, ci, 0, 0))
        down_all = lax.dynamic_update_slice(down_all, theirs, (at, 1 - ci, 0, 0))
    down_all = down_all.reshape(8 * height, -1)

    part = dot(relative(cols, xi, ci), proj_own) + dot(relative(cols, xi, 1 - ci), proj_other)
    near = sums_over_y(part)
    stream2 = residual2 + near + swap(near.astype(BF), "zh").astype(F32)
    squares = jnp.sum(stream2 * stream2, axis=(0, 2))
    scaled2 = (stream2 * gain2[:, None, :]).astype(BF)
    squares = jnp.pad(squares, (0, 256 - rows)).reshape(2, 128)
    high = exact(squares)
    tail = jnp.concatenate([high, squares - high, jnp.zeros((4, 128), F32)]).astype(BF)
    sent = jnp.concatenate([scaled2.reshape(2 * rows, 128), tail])
    arrived = from_everyone(sent, "y")
    squares = arrived[:, 2 * rows : 2 * rows + 4].astype(F32).sum(axis=0)
    squares = squares[:2] + squares[2:]
    model = arrived[:, : 2 * rows].reshape(2, 2, 2, rows, 128)
    model = model.transpose(2, 0, 1, 3, 4).reshape(4, 2, rows, 128)

    both = dot(relative(model, xi, ci), both_own) + dot(relative(model, xi, 1 - ci), both_other)
    both = both.reshape(2, half, 4 * ffw)
    got = swap(pick(both, 1 - bit0).astype(BF), "zl", 1)
    squares = squares + swap(squares, "zl", 1)
    both = (pick(both, bit0) + got.astype(F32)).reshape(half, 2, 2 * ffw)
    got = swap(pick(both, 1 - bit1, 1).astype(BF), "zl", 2)
    squares = squares + swap(squares, "zl", 2)
    both = pick(both, bit1, 1) + got.astype(F32)
    sent = lax.dynamic_slice_in_dim(both, step * (1 - bit2), top, 0)
    got = swap(sent.astype(BF), "zl", 4)
    squares = squares + swap(squares, "zl", 4)
    both = lax.dynamic_slice_in_dim(both, step * bit2, top, 0) + got.astype(F32)
    squares = lax.dynamic_slice_in_dim(squares.reshape(256), half * bit0 + step * bit2, top, 0)
    inverse = lax.rsqrt(squares / D + 1e-05)[:, None]
    gate_sum, up_sum = inverse * both[:, :ffw], inverse * both[:, ffw:]
    hidden = (jax.nn.silu(gate_sum) * up_sum).astype(BF)

    upper, lower = in_bits(hidden, swap(hidden, "zl", 4), bit2)
    hidden = jnp.concatenate([upper, lower[2 * top - half :]])
    hidden = jnp.stack(in_bits(hidden, swap(hidden, "zl", 2), bit1))
    hidden = jnp.stack(in_bits(hidden, swap(hidden, "zl", 1), bit0))
    hidden = hidden.transpose(0, 2, 1, 3).reshape(rows, 2 * ffw)

    near = sums_over_y(dot(hidden, down_all))
    far = swap(pick(near, 1 - zh).astype(BF), "zh")
    return (pick(stream2, zh) + pick(near, zh) + far.astype(F32)).astype(BF)


def solution(mesh):
    z = mesh.shape["gz"] // 4
    split = Mesh(mesh.devices.reshape(4, 2, mesh.shape["gy"], z, 4), AXES)
    gx, gz = ("x", "c"), ("zh", "y")
    in_specs = (
        P(gx, (*gz, "zl")),
        P(gx, ("zl", *gz)),
        P((*gz, *gx), "zl"),
        P(("zl", *gz)),
        P(("zl", *gx), gz),
        P(("zl", *gx), gz),
        P((*gz, *gx), "zl"),
    )
    return jax.shard_map(
        on_device, mesh=split, in_specs=in_specs, out_specs=P(gx, ("zl", *gz)), check_vma=False
    )
```

```python
import jax
import jax.numpy as jnp
from jax import lax
from jax.experimental import pallas as pl
from jax.experimental.pallas import tpu as pltpu
from jax.sharding import Mesh
from jax.sharding import PartitionSpec as P


D = 8192
BF = jnp.bfloat16
F32 = jnp.float32
AXES = ("x", "c", "zl", "zh", "y")


def shift(value, axis, step):
    n = lax.axis_size(axis)
    return lax.ppermute(value, axis, [(i, (i + step) % n) for i in range(n)])


def swap(value, axis, bit):
    n = lax.axis_size(axis)
    return lax.ppermute(value, axis, [(i, i ^ bit) for i in range(n)])


def pick(value, index, dim=0):
    return lax.dynamic_index_in_dim(value, index, dim, keepdims=False)


def exchange(parts, axis):
    return lax.all_to_all(parts, axis, split_axis=0, concat_axis=0, tiled=True)


def from_everyone(value, axis):
    copies = jnp.broadcast_to(value, (lax.axis_size(axis), *value.shape))
    return exchange(copies, axis)


def in_bits(own, other, bit):
    first = jnp.where(bit == 0, own, other)
    second = jnp.where(bit == 0, other, own)
    return first, second


def stack_kernel(*refs):
    *ins, out, sems = refs
    height = ins[0].shape[0]
    copies = [
        pltpu.make_async_copy(ref, out.at[pl.ds(k * height, height)], sems.at[k])
        for k, ref in enumerate(ins)
    ]
    for copy in copies:
        copy.start()
    for copy in copies:
        copy.wait()


def stacked(parts):
    height, width = parts[0].shape
    hbm, anywhere = pl.BlockSpec(memory_space=pltpu.HBM), pl.BlockSpec(memory_space=pl.ANY)
    return pl.pallas_call(
        stack_kernel,
        out_shape=jax.ShapeDtypeStruct((len(parts) * height, width), BF),
        in_specs=[anywhere] * len(parts),
        out_specs=hbm,
        scratch_shapes=[pltpu.SemaphoreType.DMA((len(parts),))],
        name="stack",
    )(*parts)


def gathered(w):
    parts = [w, shift(w, "x", 1), shift(w, "x", 2), shift(w, "x", -1)]
    own = stacked(parts)
    return own, swap(own, "c", 1)


def dot(a, b):
    return jnp.dot(a, b, preferred_element_type=F32)


def proj_kernel(at, x, own, other, out):
    xi, ci = at[0], at[1]
    rows = x.shape[1]
    blocks = [((xi + 4 - k) & 3) * 2 for k in range(4)]
    mine = jnp.concatenate([x[b + ci] for b in blocks], axis=1)
    theirs = jnp.concatenate([x[b + 1 - ci] for b in blocks], axis=1)
    part = (dot(mine, own[...]) + dot(theirs, other[...])).astype(BF)
    for zh in range(2):
        for y in range(4):
            n = (zh * 4 + y) * 128
            out[y, zh * rows : (zh + 1) * rows] = part[:, n : n + 128]


def proj_parts(at, x, own, other):
    rows = x.shape[1]
    vmem = pl.BlockSpec(memory_space=pltpu.VMEM)
    return pl.pallas_call(
        proj_kernel,
        out_shape=jax.ShapeDtypeStruct((4, 2 * rows, 128), BF),
        in_specs=[pl.BlockSpec(memory_space=pltpu.SMEM), vmem, vmem, vmem],
        out_specs=vmem,
        cost_estimate=pl.CostEstimate(
            flops=2 * rows * 1024 * 1024, bytes_accessed=3 << 20, transcendentals=0
        ),
        name="proj_mm",
    )(at, x, own, other)


def both_kernel(at, x, own, other, send, keep):
    xi, ci, bit = at[0], at[1], at[2]
    rows = 2 * send.shape[1]
    blocks = [(xi + 4 - k) & 3 for k in range(4)]

    def block(b, core):
        start = pl.multiple_of((b // 2) * rows, 16)
        return x[(b % 2) * 2 + core, pl.ds(start, rows)]

    mine = jnp.concatenate([block(b, ci) for b in blocks], axis=1)
    theirs = jnp.concatenate([block(b, 1 - ci) for b in blocks], axis=1)
    part = dot(mine, own[...]) + dot(theirs, other[...])
    upper, lower = part[: rows // 2], part[rows // 2 :]
    send[0] = jnp.where(bit == 0, lower, upper).astype(BF)
    keep[0] = jnp.where(bit == 0, upper, lower)


def both_parts(at, x, own, other, rows):
    depth, wide = own.shape
    tile = wide // 4
    halves = (2, rows // 2, wide // 2)
    weights = pl.BlockSpec((depth, tile), lambda n: (0, n))
    result = pl.BlockSpec((1, rows // 2, tile), lambda n: (n // 2, 0, n % 2))
    return pl.pallas_call(
        both_kernel,
        grid=(4,),
        out_shape=(jax.ShapeDtypeStruct(halves, BF), jax.ShapeDtypeStruct(halves, F32)),
        in_specs=[
            pl.BlockSpec(memory_space=pltpu.SMEM),
            pl.BlockSpec(x.shape, lambda n: (0, 0, 0)),
            weights,
            weights,
        ],
        out_specs=(result, result),
        cost_estimate=pl.CostEstimate(
            flops=4 * rows * depth * wide, bytes_accessed=9 << 20, transcendentals=0
        ),
        name="both_mm",
    )(at, x, own, other)


def down_kernel(at, x, own, other, out, whole, sems):
    xi, ci = at[0], at[1]
    rows = x.shape[0]
    height = own.shape[0] // 4
    copies = []
    for j, (ref, core) in enumerate(((own, ci), (other, 1 - ci))):
        for k in range(4):
            b = ((xi + 4 - k) & 3) * 2 + core
            to = whole.at[pl.ds(pl.multiple_of(b * height, 16), height)]
            source = ref.at[pl.ds(k * height, height)]
            copies.append(pltpu.make_async_copy(source, to, sems.at[j * 4 + k]))
    for copy in copies:
        copy.start()
    for copy in copies:
        copy.wait()
    part = dot(x[...], whole[...]).astype(BF)
    for zh in range(2):
        for y in range(4):
            n = (zh * 4 + y) * 128
            out[y, zh * rows : (zh + 1) * rows] = part[:, n : n + 128]


def down_parts(at, x, own, other):
    rows, depth = x.shape
    vmem, hbm = pl.BlockSpec(memory_space=pltpu.VMEM), pl.BlockSpec(memory_space=pltpu.HBM)
    return pl.pallas_call(
        down_kernel,
        out_shape=jax.ShapeDtypeStruct((4, 2 * rows, 128), BF),
        in_specs=[pl.BlockSpec(memory_space=pltpu.SMEM), vmem, hbm, hbm],
        out_specs=vmem,
        scratch_shapes=[pltpu.VMEM((depth, 1024), BF), pltpu.SemaphoreType.DMA((8,))],
        cost_estimate=pl.CostEstimate(
            flops=2 * rows * depth * 1024, bytes_accessed=5 << 20, transcendentals=0
        ),
        name="down_mm",
    )(at, x, own, other)


def exact(value):
    return lax.reduce_precision(value, 8, 7)


def on_device(attn_out, residual, proj_weight, norm_gain, gate_proj, up_proj, down_proj):
    xi, ci = lax.axis_index("x"), lax.axis_index("c")
    zl, zh = lax.axis_index("zl"), lax.axis_index("zh")
    bit0, bit1, bit2 = zl & 1, (zl >> 1) & 1, (zl >> 2) & 1
    at = jnp.stack([xi, ci, bit0]).astype(jnp.int32)
    rows = attn_out.shape[0]
    half = rows // 2
    top = 48
    step = half - top
    ffw = gate_proj.shape[1] // 2

    cols = from_everyone(attn_out, "zl")
    proj_own, proj_other = gathered(proj_weight)
    pieces = [gate_proj[:, :ffw], up_proj[:, :ffw], gate_proj[:, ffw:], up_proj[:, ffw:]]
    both_own, both_other = gathered(jnp.concatenate(pieces, axis=1))
    down_own, down_other = gathered(down_proj)

    high = exact(norm_gain)
    mid = exact(norm_gain - high)
    low = norm_gain - high - mid
    gains = jnp.stack([high, mid, low]).astype(BF)
    sent = jnp.concatenate([residual, jnp.pad(gains, ((0, 5), (0, 0)))])
    facing = swap(sent, "zh", 1)
    other_gain = facing[rows : rows + 3].astype(F32).sum(axis=0)
    residual2 = jnp.concatenate(in_bits(residual, facing[:rows], zh)).astype(F32)
    gain2 = jnp.repeat(jnp.stack(in_bits(norm_gain, other_gain, zh)), rows, axis=0)

    part = proj_parts(at, cols, proj_own, proj_other)
    near = exchange(part, "y").astype(F32).sum(axis=0)
    stream2 = residual2 + near + swap(near.astype(BF), "zh", 1).astype(F32)
    squares = jnp.sum((stream2 * stream2).reshape(2, rows, 128), axis=(0, 2))
    scaled2 = (stream2 * gain2).astype(BF)
    squares = jnp.pad(squares, (0, 256 - rows)).reshape(2, 128)
    high = exact(squares)
    tail = jnp.concatenate([high, squares - high, jnp.zeros((4, 128), F32)]).astype(BF)
    model = from_everyone(jnp.concatenate([scaled2, tail]), "y")
    squares = model[:, 2 * rows : 2 * rows + 4].astype(F32).sum(axis=0)
    squares = squares[:2] + squares[2:]

    send, keep = both_parts(at, model, both_own, both_other, rows)
    got = swap(send, "zl", 1).astype(F32)
    squares = squares + swap(squares, "zl", 1)
    sent = (pick(keep, 1 - bit1) + pick(got, 1 - bit1)).astype(BF)
    keep = pick(keep, bit1) + pick(got, bit1)
    got = swap(sent, "zl", 2).astype(F32)
    squares = squares + swap(squares, "zl", 2)
    both = keep + got
    sent = lax.dynamic_slice_in_dim(both, step * (1 - bit2), top, 0).astype(BF)
    got = swap(sent, "zl", 4).astype(F32)
    squares = squares + swap(squares, "zl", 4)
    both = lax.dynamic_slice_in_dim(both, step * bit2, top, 0) + got
    squares = lax.dynamic_slice_in_dim(squares.reshape(256), half * bit0 + step * bit2, top, 0)
    inverse = lax.rsqrt(squares / D + 1e-05)[:, None]
    gate_sum, up_sum = inverse * both[:, :ffw], inverse * both[:, ffw:]
    hidden = (jax.nn.silu(gate_sum) * up_sum).astype(BF)

    upper, lower = in_bits(hidden, swap(hidden, "zl", 4), bit2)
    hidden = jnp.concatenate([upper, lower[2 * top - half :]])
    hidden = jnp.concatenate(in_bits(hidden, swap(hidden, "zl", 2), bit1), axis=1)
    hidden = jnp.concatenate(in_bits(hidden, swap(hidden, "zl", 1), bit0))

    part = down_parts(at, hidden, down_own, down_other)
    near = exchange(part, "y").astype(F32).sum(axis=0).reshape(2, rows, 128)
    far = swap(pick(near, 1 - zh).astype(BF), "zh", 1)
    stream = pick(stream2.reshape(2, rows, 128), zh)
    return (stream + pick(near, zh) + far.astype(F32)).astype(BF)


def solution(mesh):
    z = mesh.shape["gz"] // 4
    split = Mesh(mesh.devices.reshape(4, 2, mesh.shape["gy"], z, 4), AXES)
    gx, gz = ("x", "c"), ("zh", "y")
    in_specs = (
        P(gx, (*gz, "zl")),
        P(gx, ("zl", *gz)),
        P((*gz, *gx), "zl"),
        P(("zl", *gz)),
        P(("zl", *gx), gz),
        P(("zl", *gx), gz),
        P((*gz, *gx), "zl"),
    )
    return jax.shard_map(
        on_device, mesh=split, in_specs=in_specs, out_specs=P(gx, ("zl", *gz)), check_vma=False
    )
```

```python
import jax
import jax.numpy as jnp
from jax import lax
from jax.experimental import pallas as pl
from jax.experimental.pallas import tpu as pltpu
from jax.sharding import Mesh
from jax.sharding import PartitionSpec as P


D = 8192
BF = jnp.bfloat16
F32 = jnp.float32
AXES = ("x", "c", "zl", "zh", "y")


def shift(value, axis, step):
    n = lax.axis_size(axis)
    return lax.ppermute(value, axis, [(i, (i + step) % n) for i in range(n)])


def swap(value, axis, bit):
    n = lax.axis_size(axis)
    return lax.ppermute(value, axis, [(i, i ^ bit) for i in range(n)])


def pick(value, index, dim=0):
    return lax.dynamic_index_in_dim(value, index, dim, keepdims=False)


def exchange(parts, axis):
    return lax.all_to_all(parts, axis, split_axis=0, concat_axis=0, tiled=True)


def from_everyone(value, axis):
    copies = jnp.broadcast_to(value, (lax.axis_size(axis), *value.shape))
    return exchange(copies, axis)


def in_bits(own, other, bit):
    first = jnp.where(bit == 0, own, other)
    second = jnp.where(bit == 0, other, own)
    return first, second


def stack_kernel(*refs):
    *ins, out = refs
    height = ins[0].shape[0]
    for k, ref in enumerate(ins):
        out[k * height : (k + 1) * height] = ref[...]


def stacked(parts):
    height, width = parts[0].shape
    vmem = pl.BlockSpec(memory_space=pltpu.VMEM)
    return pl.pallas_call(
        stack_kernel,
        out_shape=jax.ShapeDtypeStruct((len(parts) * height, width), BF),
        in_specs=[vmem] * len(parts),
        out_specs=vmem,
        name="stack",
    )(*parts)


def gathered(w):
    parts = [w, shift(w, "x", 1), shift(w, "x", 2), shift(w, "x", -1)]
    own = stacked(parts)
    return own, swap(own, "c", 1)


def dot(a, b):
    return jnp.dot(a, b, preferred_element_type=F32)


def proj_kernel(at, x, own, other, out):
    xi, ci = at[0], at[1]
    rows = x.shape[1]
    blocks = [((xi + 4 - k) & 3) * 2 for k in range(4)]
    mine = jnp.concatenate([x[b + ci] for b in blocks], axis=1)
    theirs = jnp.concatenate([x[b + 1 - ci] for b in blocks], axis=1)
    part = (dot(mine, own[...]) + dot(theirs, other[...])).astype(BF)
    for zh in range(2):
        for y in range(4):
            n = (zh * 4 + y) * 128
            out[y, zh * rows : (zh + 1) * rows] = part[:, n : n + 128]


def proj_parts(at, x, own, other):
    rows = x.shape[1]
    vmem = pl.BlockSpec(memory_space=pltpu.VMEM)
    return pl.pallas_call(
        proj_kernel,
        out_shape=jax.ShapeDtypeStruct((4, 2 * rows, 128), BF),
        in_specs=[pl.BlockSpec(memory_space=pltpu.SMEM), vmem, vmem, vmem],
        out_specs=vmem,
        cost_estimate=pl.CostEstimate(
            flops=2 * rows * 1024 * 1024, bytes_accessed=3 << 20, transcendentals=0
        ),
        name="proj_mm",
    )(at, x, own, other)


def both_kernel(at, x, own, other, send, keep):
    xi, ci, bit = at[0], at[1], at[2]
    rows = 2 * send.shape[1]
    blocks = [(xi + 4 - k) & 3 for k in range(4)]

    def block(b, core):
        start = pl.multiple_of((b // 2) * rows, 16)
        return x[(b % 2) * 2 + core, pl.ds(start, rows)]

    mine = jnp.concatenate([block(b, ci) for b in blocks], axis=1)
    theirs = jnp.concatenate([block(b, 1 - ci) for b in blocks], axis=1)
    part = dot(mine, own[...]) + dot(theirs, other[...])
    upper, lower = part[: rows // 2], part[rows // 2 :]
    send[0] = jnp.where(bit == 0, lower, upper).astype(BF)
    keep[0] = jnp.where(bit == 0, upper, lower)


def both_parts(at, x, own, other, rows):
    depth, wide = own.shape
    tile = wide // 4
    halves = (2, rows // 2, wide // 2)
    weights = pl.BlockSpec((depth, tile), lambda n: (0, n))
    result = pl.BlockSpec((1, rows // 2, tile), lambda n: (n // 2, 0, n % 2))
    return pl.pallas_call(
        both_kernel,
        grid=(4,),
        out_shape=(jax.ShapeDtypeStruct(halves, BF), jax.ShapeDtypeStruct(halves, F32)),
        in_specs=[
            pl.BlockSpec(memory_space=pltpu.SMEM),
            pl.BlockSpec(x.shape, lambda n: (0, 0, 0)),
            weights,
            weights,
        ],
        out_specs=(result, result),
        cost_estimate=pl.CostEstimate(
            flops=4 * rows * depth * wide, bytes_accessed=9 << 20, transcendentals=0
        ),
        name="both_mm",
    )(at, x, own, other)


def down_kernel(at, x, own, other, out, whole, sems):
    xi, ci = at[0], at[1]
    rows = x.shape[0]
    height = own.shape[0] // 4
    copies = []
    for j, (ref, core) in enumerate(((own, ci), (other, 1 - ci))):
        for k in range(4):
            b = ((xi + 4 - k) & 3) * 2 + core
            to = whole.at[pl.ds(pl.multiple_of(b * height, 16), height)]
            source = ref.at[pl.ds(k * height, height)]
            copies.append(pltpu.make_async_copy(source, to, sems.at[j * 4 + k]))
    for copy in copies:
        copy.start()
    for copy in copies:
        copy.wait()
    part = dot(x[...], whole[...]).astype(BF)
    for zh in range(2):
        for y in range(4):
            n = (zh * 4 + y) * 128
            out[y, zh * rows : (zh + 1) * rows] = part[:, n : n + 128]


def down_parts(at, x, own, other):
    rows, depth = x.shape
    vmem, hbm = pl.BlockSpec(memory_space=pltpu.VMEM), pl.BlockSpec(memory_space=pltpu.HBM)
    return pl.pallas_call(
        down_kernel,
        out_shape=jax.ShapeDtypeStruct((4, 2 * rows, 128), BF),
        in_specs=[pl.BlockSpec(memory_space=pltpu.SMEM), vmem, hbm, hbm],
        out_specs=vmem,
        scratch_shapes=[pltpu.VMEM((depth, 1024), BF), pltpu.SemaphoreType.DMA((8,))],
        cost_estimate=pl.CostEstimate(
            flops=2 * rows * depth * 1024, bytes_accessed=5 << 20, transcendentals=0
        ),
        name="down_mm",
    )(at, x, own, other)


def exact(value):
    return lax.reduce_precision(value, 8, 7)


def on_device(attn_out, residual, proj_weight, norm_gain, gate_proj, up_proj, down_proj):
    xi, ci = lax.axis_index("x"), lax.axis_index("c")
    zl, zh = lax.axis_index("zl"), lax.axis_index("zh")
    bit0, bit1, bit2 = zl & 1, (zl >> 1) & 1, (zl >> 2) & 1
    at = jnp.stack([xi, ci, bit0]).astype(jnp.int32)
    rows = attn_out.shape[0]
    half = rows // 2
    top = 48
    step = half - top
    ffw = gate_proj.shape[1] // 2

    cols = from_everyone(attn_out, "zl")
    proj_own, proj_other = gathered(proj_weight)
    pieces = [gate_proj[:, :ffw], up_proj[:, :ffw], gate_proj[:, ffw:], up_proj[:, ffw:]]
    both_own, both_other = gathered(jnp.concatenate(pieces, axis=1))
    down_own, down_other = gathered(down_proj)

    high = exact(norm_gain)
    mid = exact(norm_gain - high)
    low = norm_gain - high - mid
    gains = jnp.stack([high, mid, low]).astype(BF)
    sent = jnp.concatenate([residual, jnp.pad(gains, ((0, 5), (0, 0)))])
    facing = swap(sent, "zh", 1)
    other_gain = facing[rows : rows + 3].astype(F32).sum(axis=0)
    residual2 = jnp.concatenate(in_bits(residual, facing[:rows], zh)).astype(F32)
    gain2 = jnp.repeat(jnp.stack(in_bits(norm_gain, other_gain, zh)), rows, axis=0)

    part = proj_parts(at, cols, proj_own, proj_other)
    near = exchange(part, "y").astype(F32).sum(axis=0)
    stream2 = residual2 + near + swap(near.astype(BF), "zh", 1).astype(F32)
    squares = jnp.sum((stream2 * stream2).reshape(2, rows, 128), axis=(0, 2))
    scaled2 = (stream2 * gain2).astype(BF)
    squares = jnp.pad(squares, (0, 256 - rows)).reshape(2, 128)
    high = exact(squares)
    tail = jnp.concatenate([high, squares - high, jnp.zeros((4, 128), F32)]).astype(BF)
    model = from_everyone(jnp.concatenate([scaled2, tail]), "y")
    squares = model[:, 2 * rows : 2 * rows + 4].astype(F32).sum(axis=0)
    squares = squares[:2] + squares[2:]

    send, keep = both_parts(at, model, both_own, both_other, rows)
    got = swap(send, "zl", 1).astype(F32)
    squares = squares + swap(squares, "zl", 1)
    sent = (pick(keep, 1 - bit1) + pick(got, 1 - bit1)).astype(BF)
    keep = pick(keep, bit1) + pick(got, bit1)
    got = swap(sent, "zl", 2).astype(F32)
    squares = squares + swap(squares, "zl", 2)
    both = keep + got
    sent = lax.dynamic_slice_in_dim(both, step * (1 - bit2), top, 0).astype(BF)
    got = swap(sent, "zl", 4).astype(F32)
    squares = squares + swap(squares, "zl", 4)
    both = lax.dynamic_slice_in_dim(both, step * bit2, top, 0) + got
    squares = lax.dynamic_slice_in_dim(squares.reshape(256), half * bit0 + step * bit2, top, 0)
    inverse = lax.rsqrt(squares / D + 1e-05)[:, None]
    gate_sum, up_sum = inverse * both[:, :ffw], inverse * both[:, ffw:]
    hidden = (jax.nn.silu(gate_sum) * up_sum).astype(BF)

    upper, lower = in_bits(hidden, swap(hidden, "zl", 4), bit2)
    hidden = jnp.concatenate([upper, lower[2 * top - half :]])
    hidden = jnp.concatenate(in_bits(hidden, swap(hidden, "zl", 2), bit1), axis=1)
    hidden = jnp.concatenate(in_bits(hidden, swap(hidden, "zl", 1), bit0))

    part = down_parts(at, hidden, down_own, down_other)
    near = exchange(part, "y").astype(F32).sum(axis=0).reshape(2, rows, 128)
    far = swap(pick(near, 1 - zh).astype(BF), "zh", 1)
    stream = pick(stream2.reshape(2, rows, 128), zh)
    return (stream + pick(near, zh) + far.astype(F32)).astype(BF)


def solution(mesh):
    z = mesh.shape["gz"] // 4
    split = Mesh(mesh.devices.reshape(4, 2, mesh.shape["gy"], z, 4), AXES)
    gx, gz = ("x", "c"), ("zh", "y")
    in_specs = (
        P(gx, (*gz, "zl")),
        P(gx, ("zl", *gz)),
        P((*gz, *gx), "zl"),
        P(("zl", *gz)),
        P(("zl", *gx), gz),
        P(("zl", *gx), gz),
        P((*gz, *gx), "zl"),
    )
    return jax.shard_map(
        on_device, mesh=split, in_specs=in_specs, out_specs=P(gx, ("zl", *gz)), check_vma=False
    )
```

```python
import jax
import jax.numpy as jnp
from jax import lax
from jax.experimental import pallas as pl
from jax.experimental.pallas import tpu as pltpu
from jax.sharding import Mesh
from jax.sharding import PartitionSpec as P


D = 8192
BF = jnp.bfloat16
F32 = jnp.float32
AXES = ("x", "c", "zl", "zh", "y")


def shift(value, axis, step):
    n = lax.axis_size(axis)
    return lax.ppermute(value, axis, [(i, (i + step) % n) for i in range(n)])


def swap(value, axis, bit):
    n = lax.axis_size(axis)
    return lax.ppermute(value, axis, [(i, i ^ bit) for i in range(n)])


def pick(value, index, dim=0):
    return lax.dynamic_index_in_dim(value, index, dim, keepdims=False)


def exchange(parts, axis):
    return lax.all_to_all(parts, axis, split_axis=0, concat_axis=0, tiled=True)


def from_everyone(value, axis):
    copies = jnp.broadcast_to(value, (lax.axis_size(axis), *value.shape))
    return exchange(copies, axis)


def in_bits(own, other, bit):
    first = jnp.where(bit == 0, own, other)
    second = jnp.where(bit == 0, other, own)
    return first, second


def stack_kernel(*refs):
    *ins, out = refs
    height = ins[0].shape[0]
    for k, ref in enumerate(ins):
        out[k * height : (k + 1) * height] = ref[...]


def stacked(parts):
    height, width = parts[0].shape
    vmem = pl.BlockSpec(memory_space=pltpu.VMEM)
    return pl.pallas_call(
        stack_kernel,
        out_shape=jax.ShapeDtypeStruct((len(parts) * height, width), BF),
        in_specs=[vmem] * len(parts),
        out_specs=vmem,
        name="stack",
    )(*parts)


def gathered(w):
    parts = [w, shift(w, "x", 1), shift(w, "x", 2), shift(w, "x", -1)]
    own = stacked(parts)
    return own, swap(own, "c", 1)


def dot(a, b):
    return jnp.dot(a, b, preferred_element_type=F32)


def proj_kernel(at, x, own, other, out):
    xi, ci, zl = at[0], at[1], at[2]
    rows = x.shape[1]

    def block(b):
        off = b ^ zl
        return x[((off >> 2) & 1) | (off & 2) | ((off & 1) << 2)]

    blocks = [((xi + 4 - k) & 3) * 2 for k in range(4)]
    mine = jnp.concatenate([block(b + ci) for b in blocks], axis=1)
    theirs = jnp.concatenate([block(b + 1 - ci) for b in blocks], axis=1)
    part = (dot(mine, own[...]) + dot(theirs, other[...])).astype(BF)
    for zh in range(2):
        for y in range(4):
            n = (zh * 4 + y) * 128
            out[y, zh * rows : (zh + 1) * rows] = part[:, n : n + 128]


def proj_parts(at, x, own, other):
    rows = x.shape[1]
    vmem = pl.BlockSpec(memory_space=pltpu.VMEM)
    return pl.pallas_call(
        proj_kernel,
        out_shape=jax.ShapeDtypeStruct((4, 2 * rows, 128), BF),
        in_specs=[pl.BlockSpec(memory_space=pltpu.SMEM), vmem, vmem, vmem],
        out_specs=vmem,
        cost_estimate=pl.CostEstimate(
            flops=2 * rows * 1024 * 1024, bytes_accessed=3 << 20, transcendentals=0
        ),
        name="proj_mm",
    )(at, x, own, other)


def both_kernel(at, x, own, other, send, keep):
    xi, ci, bit = at[0], at[1], at[2] & 1
    rows = 2 * send.shape[1]
    blocks = [(xi + 4 - k) & 3 for k in range(4)]

    def block(b, core):
        start = pl.multiple_of((b // 2) * rows, 16)
        return x[(b % 2) * 2 + core, pl.ds(start, rows)]

    mine = jnp.concatenate([block(b, ci) for b in blocks], axis=1)
    theirs = jnp.concatenate([block(b, 1 - ci) for b in blocks], axis=1)
    part = dot(mine, own[...]) + dot(theirs, other[...])
    upper, lower = part[: rows // 2], part[rows // 2 :]
    send[0] = jnp.where(bit == 0, lower, upper).astype(BF)
    keep[0] = jnp.where(bit == 0, upper, lower)


def both_parts(at, x, own, other, rows):
    depth, wide = own.shape
    tile = wide // 4
    halves = (2, rows // 2, wide // 2)
    weights = pl.BlockSpec((depth, tile), lambda n: (0, n))
    result = pl.BlockSpec((1, rows // 2, tile), lambda n: (n // 2, 0, n % 2))
    return pl.pallas_call(
        both_kernel,
        grid=(4,),
        out_shape=(jax.ShapeDtypeStruct(halves, BF), jax.ShapeDtypeStruct(halves, F32)),
        in_specs=[
            pl.BlockSpec(memory_space=pltpu.SMEM),
            pl.BlockSpec(x.shape, lambda n: (0, 0, 0)),
            weights,
            weights,
        ],
        out_specs=(result, result),
        cost_estimate=pl.CostEstimate(
            flops=4 * rows * depth * wide, bytes_accessed=9 << 20, transcendentals=0
        ),
        name="both_mm",
    )(at, x, own, other)


def down_kernel(at, x, own, other, out, whole):
    xi, ci = at[0], at[1]
    rows = x.shape[0]
    height = own.shape[0] // 4
    for ref, core in ((own, ci), (other, 1 - ci)):
        for k in range(4):
            b = ((xi + 4 - k) & 3) * 2 + core
            to = pl.ds(pl.multiple_of(b * height, 16), height)
            whole[to] = ref[k * height : (k + 1) * height]
    part = dot(x[...], whole[...]).astype(BF)
    for zh in range(2):
        for y in range(4):
            n = (zh * 4 + y) * 128
            out[y, zh * rows : (zh + 1) * rows] = part[:, n : n + 128]


def down_parts(at, x, own, other):
    rows, depth = x.shape
    vmem = pl.BlockSpec(memory_space=pltpu.VMEM)
    return pl.pallas_call(
        down_kernel,
        out_shape=jax.ShapeDtypeStruct((4, 2 * rows, 128), BF),
        in_specs=[pl.BlockSpec(memory_space=pltpu.SMEM), vmem, vmem, vmem],
        out_specs=vmem,
        scratch_shapes=[pltpu.VMEM((depth, 1024), BF)],
        cost_estimate=pl.CostEstimate(
            flops=2 * rows * depth * 1024, bytes_accessed=5 << 20, transcendentals=0
        ),
        name="down_mm",
    )(at, x, own, other)


def exact(value):
    return lax.reduce_precision(value, 8, 7)


def on_device(attn_out, residual, proj_weight, norm_gain, gate_proj, up_proj, down_proj):
    xi, ci = lax.axis_index("x"), lax.axis_index("c")
    zl, zh = lax.axis_index("zl"), lax.axis_index("zh")
    bit0, bit1, bit2 = zl & 1, (zl >> 1) & 1, (zl >> 2) & 1
    at = jnp.stack([xi, ci, zl]).astype(jnp.int32)
    rows = attn_out.shape[0]
    half = rows // 2
    top = 48
    step = half - top
    ffw = gate_proj.shape[1] // 2

    cols = attn_out[None]
    for step_bit in (4, 2, 1):
        cols = jnp.concatenate([cols, swap(cols, "zl", step_bit)])
    proj_own, proj_other = gathered(proj_weight)
    pieces = [gate_proj[:, :ffw], up_proj[:, :ffw], gate_proj[:, ffw:], up_proj[:, ffw:]]
    both_own, both_other = gathered(jnp.concatenate(pieces, axis=1))
    down_own, down_other = gathered(down_proj)

    high = exact(norm_gain)
    mid = exact(norm_gain - high)
    low = norm_gain - high - mid
    gains = jnp.pad(jnp.stack([high, mid, low]), ((0, 5), (0, 0)))

    part = proj_parts(at, cols, proj_own, proj_other)
    near = exchange(part, "y").astype(F32).sum(axis=0).reshape(2, rows, 128)
    mine = jnp.arange(2)[:, None, None] == zh
    near = jnp.where(mine, near + residual.astype(F32), near).reshape(2 * rows, 128)
    far = swap(jnp.concatenate([near, gains]).astype(BF), "zh", 1).astype(F32)
    stream2 = near + far[: 2 * rows]
    other_gain = far[2 * rows : 2 * rows + 3].sum(axis=0)
    gain2 = jnp.repeat(jnp.stack(in_bits(norm_gain, other_gain, zh)), rows, axis=0)
    squares = jnp.sum((stream2 * stream2).reshape(2, rows, 128), axis=(0, 2))
    scaled2 = (stream2 * gain2).astype(BF)
    squares = jnp.pad(squares, (0, 256 - rows)).reshape(2, 128)
    high = exact(squares)
    tail = jnp.concatenate([high, squares - high, jnp.zeros((4, 128), F32)]).astype(BF)
    model = from_everyone(jnp.concatenate([scaled2, tail]), "y")
    squares = model[:, 2 * rows : 2 * rows + 4].astype(F32).sum(axis=0)
    squares = squares[:2] + squares[2:]

    send, keep = both_parts(at, model, both_own, both_other, rows)
    got = swap(send, "zl", 1).astype(F32)
    squares = squares + swap(squares, "zl", 1)
    sent = (pick(keep, 1 - bit1) + pick(got, 1 - bit1)).astype(BF)
    keep = pick(keep, bit1) + pick(got, bit1)
    got = swap(sent, "zl", 2).astype(F32)
    squares = squares + swap(squares, "zl", 2)
    both = keep + got
    sent = lax.dynamic_slice_in_dim(both, step * (1 - bit2), top, 0).astype(BF)
    got = swap(sent, "zl", 4).astype(F32)
    squares = squares + swap(squares, "zl", 4)
    both = lax.dynamic_slice_in_dim(both, step * bit2, top, 0) + got
    squares = lax.dynamic_slice_in_dim(squares.reshape(256), half * bit0 + step * bit2, top, 0)
    inverse = lax.rsqrt(squares / D + 1e-05)[:, None]
    gate_sum, up_sum = inverse * both[:, :ffw], inverse * both[:, ffw:]
    hidden = (jax.nn.silu(gate_sum) * up_sum).astype(BF)

    upper, lower = in_bits(hidden, swap(hidden, "zl", 4), bit2)
    hidden = jnp.concatenate([upper, lower[2 * top - half :]])
    hidden = jnp.concatenate(in_bits(hidden, swap(hidden, "zl", 2), bit1), axis=1)
    hidden = jnp.concatenate(in_bits(hidden, swap(hidden, "zl", 1), bit0))

    part = down_parts(at, hidden, down_own, down_other)
    near = exchange(part, "y").astype(F32).sum(axis=0).reshape(2, rows, 128)
    far = swap(pick(near, 1 - zh).astype(BF), "zh", 1)
    stream = pick(stream2.reshape(2, rows, 128), zh)
    return (stream + pick(near, zh) + far.astype(F32)).astype(BF)


def solution(mesh):
    z = mesh.shape["gz"] // 4
    split = Mesh(mesh.devices.reshape(4, 2, mesh.shape["gy"], z, 4), AXES)
    gx, gz = ("x", "c"), ("zh", "y")
    in_specs = (
        P(gx, (*gz, "zl")),
        P(gx, ("zl", *gz)),
        P((*gz, *gx), "zl"),
        P(("zl", *gz)),
        P(("zl", *gx), gz),
        P(("zl", *gx), gz),
        P((*gz, *gx), "zl"),
    )
    return jax.shard_map(
        on_device, mesh=split, in_specs=in_specs, out_specs=P(gx, ("zl", *gz)), check_vma=False
    )
```

```python
import jax
import jax.numpy as jnp
from jax import lax
from jax.experimental import pallas as pl
from jax.experimental.pallas import tpu as pltpu
from jax.sharding import Mesh
from jax.sharding import PartitionSpec as P


D = 8192
BF = jnp.bfloat16
F32 = jnp.float32
AXES = ("x", "c", "zl", "zh", "y")


def swap(value, axis, bit):
    n = lax.axis_size(axis)
    return lax.ppermute(value, axis, [(i, i ^ bit) for i in range(n)])


def pick(value, index, dim=0):
    return lax.dynamic_index_in_dim(value, index, dim, keepdims=False)


def exchange(parts, axis):
    return lax.all_to_all(parts, axis, split_axis=0, concat_axis=0, tiled=True)


def from_everyone(value, axis):
    copies = jnp.broadcast_to(value, (lax.axis_size(axis), *value.shape))
    return exchange(copies, axis)


def in_bits(own, other, bit):
    first = jnp.where(bit == 0, own, other)
    second = jnp.where(bit == 0, other, own)
    return first, second


def gathered(w):
    own = from_everyone(w, "x").reshape(-1, w.shape[1])
    return own, swap(own, "c", 1)


def dot(a, b):
    return jnp.dot(a, b, preferred_element_type=F32)


def proj_kernel(at, x, own, other, *outs):
    ci, zl, yi = at[0], at[2], at[3]
    rows = x.shape[1]

    def blocks(core):
        offs = [(2 * k + core) ^ zl for k in range(4)]
        return [x[((off >> 2) & 1) | (off & 2) | ((off & 1) << 2)] for off in offs]

    mine = jnp.concatenate(blocks(ci), axis=1)
    theirs = jnp.concatenate(blocks(1 - ci), axis=1)
    part = (dot(mine, own[...]) + dot(theirs, other[...])).astype(BF)
    *outs, parts = outs
    for zh in range(2):
        for y in range(4):
            n = (zh * 4 + y) * 128
            parts[y, zh * rows : (zh + 1) * rows] = part[:, n : n + 128]
    for k, out in enumerate(outs):
        out[...] = parts[yi ^ k]


def proj_parts(at, x, own, other):
    rows = x.shape[1]
    vmem = pl.BlockSpec(memory_space=pltpu.VMEM)
    return pl.pallas_call(
        proj_kernel,
        out_shape=[jax.ShapeDtypeStruct((2 * rows, 128), BF)] * 4,
        in_specs=[pl.BlockSpec(memory_space=pltpu.SMEM), vmem, vmem, vmem],
        out_specs=[vmem] * 4,
        scratch_shapes=[pltpu.VMEM((4, 2 * rows, 128), BF)],
        cost_estimate=pl.CostEstimate(
            flops=2 * rows * 1024 * 1024, bytes_accessed=3 << 20, transcendentals=0
        ),
        name="proj_mm",
    )(at, x, own, other)


def both_kernel(at, x0, x1, x2, x3, own, other, send, keep, x):
    ci, bit, yi = at[0], at[1], at[3]
    rows = 2 * send.shape[1]

    @pl.when(pl.program_id(0) == 0)
    def _():
        for k, ref in enumerate((x0, x1, x2, x3)):
            x[yi ^ k] = ref[...]

    def blocks(core):
        parts = [x[(k % 2) * 2 + core, pl.ds((k // 2) * rows, rows)] for k in range(4)]
        return jnp.concatenate(parts, axis=1)

    mine, theirs = blocks(ci), blocks(1 - ci)
    part = dot(mine, own[...]) + dot(theirs, other[...])
    upper, lower = part[: rows // 2], part[rows // 2 :]
    send[0] = jnp.where(bit == 0, lower, upper).astype(BF)
    keep[0] = jnp.where(bit == 0, upper, lower)


def both_parts(at, xs, own, other, rows):
    depth, wide = own.shape
    tile = wide // 4
    halves = (2, rows // 2, wide // 2)
    model = pl.BlockSpec(memory_space=pltpu.VMEM)
    weights = pl.BlockSpec((depth, tile), lambda n: (0, n))
    result = pl.BlockSpec((1, rows // 2, tile), lambda n: (n // 2, 0, n % 2))
    return pl.pallas_call(
        both_kernel,
        grid=(4,),
        out_shape=(jax.ShapeDtypeStruct(halves, BF), jax.ShapeDtypeStruct(halves, F32)),
        in_specs=[pl.BlockSpec(memory_space=pltpu.SMEM)] + [model] * 4 + [weights] * 2,
        out_specs=(result, result),
        scratch_shapes=[pltpu.VMEM((4, *xs[0].shape), BF)],
        cost_estimate=pl.CostEstimate(
            flops=4 * rows * depth * wide, bytes_accessed=9 << 20, transcendentals=0
        ),
        name="both_mm",
    )(at, *xs, own, other)


def down_kernel(at, x, own, other, out, whole):
    ci = at[0]
    rows = x.shape[0]
    height = own.shape[0] // 4
    for ref, core in ((own, ci), (other, 1 - ci)):
        for k in range(4):
            b = 2 * k + core
            to = pl.ds(pl.multiple_of(b * height, 16), height)
            whole[to] = ref[k * height : (k + 1) * height]
    part = dot(x[...], whole[...]).astype(BF)
    for zh in range(2):
        for y in range(4):
            n = (zh * 4 + y) * 128
            out[y, zh * rows : (zh + 1) * rows] = part[:, n : n + 128]


def down_parts(at, x, own, other):
    rows, depth = x.shape
    vmem = pl.BlockSpec(memory_space=pltpu.VMEM)
    return pl.pallas_call(
        down_kernel,
        out_shape=jax.ShapeDtypeStruct((4, 2 * rows, 128), BF),
        in_specs=[pl.BlockSpec(memory_space=pltpu.SMEM), vmem, vmem, vmem],
        out_specs=vmem,
        scratch_shapes=[pltpu.VMEM((depth, 1024), BF)],
        cost_estimate=pl.CostEstimate(
            flops=2 * rows * depth * 1024, bytes_accessed=5 << 20, transcendentals=0
        ),
        name="down_mm",
    )(at, x, own, other)


def exact(value):
    return lax.reduce_precision(value, 8, 7)


def on_device(attn_out, residual, proj_weight, norm_gain, gate_proj, up_proj, down_proj):
    ci, zl, zh = lax.axis_index("c"), lax.axis_index("zl"), lax.axis_index("zh")
    yi = lax.axis_index("y")
    bit0, bit1, bit2 = zl & 1, (zl >> 1) & 1, (zl >> 2) & 1
    at = jnp.stack([ci, bit0, zl, yi]).astype(jnp.int32)
    rows = attn_out.shape[0]
    half = rows // 2
    top = 48
    step = half - top
    ffw = gate_proj.shape[1] // 2

    cols = attn_out[None]
    for step_bit in (4, 2, 1):
        cols = jnp.concatenate([cols, swap(cols, "zl", step_bit)])
    proj_own, proj_other = gathered(proj_weight)
    pieces = [gate_proj[:, :ffw], up_proj[:, :ffw], gate_proj[:, ffw:], up_proj[:, ffw:]]
    both_own, both_other = gathered(jnp.concatenate(pieces, axis=1))
    down_own, down_other = gathered(down_proj)

    high = exact(norm_gain)
    mid = exact(norm_gain - high)
    low = norm_gain - high - mid
    gains = jnp.pad(jnp.stack([high, mid, low]), ((0, 5), (0, 0)))

    part = proj_parts(at, cols, proj_own, proj_other)
    near = [part[0]] + [swap(part[k], "y", k) for k in (1, 2, 3)]
    near = sum(p.astype(F32) for p in near).reshape(2, rows, 128)
    mine = jnp.arange(2)[:, None, None] == zh
    near = jnp.where(mine, near + residual.astype(F32), near).reshape(2 * rows, 128)
    far = swap(jnp.concatenate([near, gains]).astype(BF), "zh", 1).astype(F32)
    stream2 = near + far[: 2 * rows]
    other_gain = far[2 * rows : 2 * rows + 3].sum(axis=0)
    gain2 = jnp.repeat(jnp.stack(in_bits(norm_gain, other_gain, zh)), rows, axis=0)
    squares = jnp.sum((stream2 * stream2).reshape(2, rows, 128), axis=(0, 2))
    scaled2 = (stream2 * gain2).astype(BF)
    squares = jnp.pad(squares, (0, 256 - rows)).reshape(2, 128)
    high = exact(squares)
    tail = jnp.concatenate([high, squares - high, jnp.zeros((4, 128), F32)]).astype(BF)
    model = jnp.concatenate([scaled2, tail])
    model = [model] + [swap(model, "y", k) for k in (1, 2, 3)]
    squares = sum(m[2 * rows : 2 * rows + 4].astype(F32) for m in model)
    squares = squares[:2] + squares[2:]

    send, keep = both_parts(at, model, both_own, both_other, rows)
    got = swap(send, "zl", 1).astype(F32)
    squares = squares + swap(squares, "zl", 1)
    sent = (pick(keep, 1 - bit1) + pick(got, 1 - bit1)).astype(BF)
    keep = pick(keep, bit1) + pick(got, bit1)
    got = swap(sent, "zl", 2).astype(F32)
    squares = squares + swap(squares, "zl", 2)
    both = keep + got
    sent = lax.dynamic_slice_in_dim(both, step * (1 - bit2), top, 0).astype(BF)
    got = swap(sent, "zl", 4).astype(F32)
    squares = squares + swap(squares, "zl", 4)
    both = lax.dynamic_slice_in_dim(both, step * bit2, top, 0) + got
    squares = lax.dynamic_slice_in_dim(squares.reshape(256), half * bit0 + step * bit2, top, 0)
    inverse = lax.rsqrt(squares / D + 1e-05)[:, None]
    gate_sum, up_sum = inverse * both[:, :ffw], inverse * both[:, ffw:]
    hidden = (jax.nn.silu(gate_sum) * up_sum).astype(BF)

    upper, lower = in_bits(hidden, swap(hidden, "zl", 4), bit2)
    hidden = jnp.concatenate([upper, lower[2 * top - half :]])
    hidden = jnp.concatenate(in_bits(hidden, swap(hidden, "zl", 2), bit1), axis=1)
    hidden = jnp.concatenate(in_bits(hidden, swap(hidden, "zl", 1), bit0))

    part = down_parts(at, hidden, down_own, down_other)
    near = exchange(part, "y").astype(F32).sum(axis=0).reshape(2, rows, 128)
    far = swap(pick(near, 1 - zh).astype(BF), "zh", 1)
    stream = pick(stream2.reshape(2, rows, 128), zh)
    return (stream + pick(near, zh) + far.astype(F32)).astype(BF)


def solution(mesh):
    z = mesh.shape["gz"] // 4
    split = Mesh(mesh.devices.reshape(4, 2, mesh.shape["gy"], z, 4), AXES)
    gx, gz = ("x", "c"), ("zh", "y")
    in_specs = (
        P(gx, (*gz, "zl")),
        P(gx, ("zl", *gz)),
        P((*gz, *gx), "zl"),
        P(("zl", *gz)),
        P(("zl", *gx), gz),
        P(("zl", *gx), gz),
        P((*gz, *gx), "zl"),
    )
    return jax.shard_map(
        on_device, mesh=split, in_specs=in_specs, out_specs=P(gx, ("zl", *gz)), check_vma=False
    )
```

```python
import jax
import jax.numpy as jnp
from jax import lax
from jax.experimental import pallas as pl
from jax.experimental.pallas import tpu as pltpu
from jax.sharding import Mesh
from jax.sharding import PartitionSpec as P


D = 8192
BF = jnp.bfloat16
F32 = jnp.float32
AXES = ("x", "c", "zq", "zp", "zh", "y")
ZL = ("zq", "zp")
TOP = 48
STARTS_OF = (0, 48, 88, 128)
SPANS = ((0, 0, 48), (1, 48, 96), (2, 96, 136), (3, 136, 176))


def size_of(axis):
    return lax.axis_size(axis)


def shift(value, axis, step):
    n = size_of(axis)
    return lax.ppermute(value, axis, [(i, (i + step) % n) for i in range(n)])


def swap(value, axis, bit):
    n = size_of(axis)
    return lax.ppermute(value, axis, [(i, i ^ bit) for i in range(n)])


def pick(value, index, dim=0):
    return lax.dynamic_index_in_dim(value, index, dim, keepdims=False)


def exchange(parts, axis):
    return lax.all_to_all(parts, axis, split_axis=0, concat_axis=0, tiled=True)


def from_everyone(value, axis):
    copies = jnp.broadcast_to(value, (size_of(axis), *value.shape))
    return exchange(copies, axis)


def in_bits(own, other, bit):
    first = jnp.where(bit == 0, own, other)
    second = jnp.where(bit == 0, other, own)
    return first, second


def stack_kernel(*refs):
    *ins, out = refs
    height = ins[0].shape[0]
    for k, ref in enumerate(ins):
        out[k * height : (k + 1) * height] = ref[...]


def stacked(parts):
    height, width = parts[0].shape
    vmem = pl.BlockSpec(memory_space=pltpu.VMEM)
    return pl.pallas_call(
        stack_kernel,
        out_shape=jax.ShapeDtypeStruct((len(parts) * height, width), BF),
        in_specs=[vmem] * len(parts),
        out_specs=vmem,
        name="stack",
    )(*parts)


def dot(a, b):
    return jnp.dot(a, b, preferred_element_type=F32)


def proj_kernel(at, x, own, other, *outs):
    ci, zl, yi = at[0], at[2], at[3]
    rows = x.shape[1]

    def blocks(core):
        offs = [(2 * k + core) ^ zl for k in range(4)]
        return [x[((off >> 2) & 1) | (off & 2) | ((off & 1) << 2)] for off in offs]

    mine = jnp.concatenate(blocks(ci), axis=1)
    theirs = jnp.concatenate(blocks(1 - ci), axis=1)
    part = (dot(mine, own[...]) + dot(theirs, other[...])).astype(BF)
    *outs, parts = outs
    for zh in range(2):
        for y in range(4):
            n = (zh * 4 + y) * 128
            parts[y, zh * rows : (zh + 1) * rows] = part[:, n : n + 128]
    for k, out in enumerate(outs):
        out[...] = parts[yi ^ k]


def proj_parts(at, x, own, other):
    rows = x.shape[1]
    vmem = pl.BlockSpec(memory_space=pltpu.VMEM)
    return pl.pallas_call(
        proj_kernel,
        out_shape=[jax.ShapeDtypeStruct((2 * rows, 128), BF)] * 4,
        in_specs=[pl.BlockSpec(memory_space=pltpu.SMEM), vmem, vmem, vmem],
        out_specs=[vmem] * 4,
        scratch_shapes=[pltpu.VMEM((4, 2 * rows, 128), BF)],
        cost_estimate=pl.CostEstimate(
            flops=2 * rows * 1024 * 1024, bytes_accessed=3 << 20, transcendentals=0
        ),
        name="proj_mm",
    )(at, x, own, other)


def both_kernel(at, x, own, other, out):
    ci, zp = at[0], at[1]
    rows = (x.shape[1] - 8) // 2

    def blocks(core):
        parts = []
        for k in range(4):
            for turn in range(2):
                at_block = (zp ^ turn) * 4 + (k % 2) * 2 + core
                parts.append(x[at_block, pl.ds((k // 2) * rows, rows)])
        return jnp.concatenate(parts, axis=1)

    part = (dot(blocks(ci), own[...]) + dot(blocks(1 - ci), other[...])).astype(BF)
    for q in range(4):
        out[q] = part[STARTS_OF[q] : STARTS_OF[q] + TOP]


def both_parts(at, x, own, other):
    depth, wide = own.shape
    tile = 256
    vmem = pl.BlockSpec(memory_space=pltpu.VMEM)
    weights = pl.BlockSpec((depth, tile), lambda n: (0, n))
    return pl.pallas_call(
        both_kernel,
        grid=(wide // tile,),
        out_shape=jax.ShapeDtypeStruct((4, TOP, wide), BF),
        in_specs=[pl.BlockSpec(memory_space=pltpu.SMEM), vmem, weights, weights],
        out_specs=pl.BlockSpec((4, TOP, tile), lambda n: (0, 0, n)),
        cost_estimate=pl.CostEstimate(
            flops=4 * 176 * depth * wide, bytes_accessed=9 << 20, transcendentals=0
        ),
        name="both_mm",
    )(at, x, own, other)


def down_kernel(at, x, own, other, out, whole):
    ci, xi = at[0], at[4]
    height = own.shape[0] // 4
    rows = x.shape[0]
    for ref, core in ((own, ci), (other, 1 - ci)):
        for k in range(4):
            b = ((xi + 4 - k) & 3) * 2 + core
            to = pl.ds(pl.multiple_of(b * height, 16), height)
            whole[to] = ref[k * height : (k + 1) * height]
    part = dot(x[...], whole[...]).astype(BF)
    for zh in range(2):
        for y in range(4):
            n = (zh * 4 + y) * 128
            out[y, zh * rows : (zh + 1) * rows] = part[:, n : n + 128]


def down_parts(at, x, own, other):
    rows, depth = x.shape
    vmem = pl.BlockSpec(memory_space=pltpu.VMEM)
    return pl.pallas_call(
        down_kernel,
        out_shape=jax.ShapeDtypeStruct((4, 2 * rows, 128), BF),
        in_specs=[pl.BlockSpec(memory_space=pltpu.SMEM), vmem, vmem, vmem],
        out_specs=vmem,
        scratch_shapes=[pltpu.VMEM((depth, 1024), BF)],
        cost_estimate=pl.CostEstimate(
            flops=2 * rows * depth * 1024, bytes_accessed=5 << 20, transcendentals=0
        ),
        name="down_mm",
    )(at, x, own, other)


def exact(value):
    return lax.reduce_precision(value, 8, 7)


def on_device(attn_out, residual, proj_weight, norm_gain, gate_proj, up_proj, down_proj):
    xi, ci, zh, yi = (lax.axis_index(name) for name in ("x", "c", "zh", "y"))
    zq, zp = lax.axis_index("zq"), lax.axis_index("zp")
    at = jnp.stack([ci, zp, 2 * zq + zp, yi, xi]).astype(jnp.int32)
    rows = attn_out.shape[0]
    ffw = gate_proj.shape[1] // 2

    cols = attn_out[None]
    for bit in (4, 2, 1):
        cols = jnp.concatenate([cols, swap(cols, ZL, bit)])

    def columns(which):
        halves = [lax.dynamic_slice_in_dim(w, which * ffw, ffw, 1) for w in (gate_proj, up_proj)]
        return jnp.concatenate(halves, axis=1)

    facing = swap(columns(1 - zp), "zp", 1)
    both = jnp.concatenate([columns(zp), facing])
    both_own = from_everyone(both, "x").reshape(-1, 2 * ffw)
    both_other = swap(both_own, "c", 1)
    proj_own = from_everyone(proj_weight, "x").reshape(-1, proj_weight.shape[1])
    proj_other = swap(proj_own, "c", 1)
    ring = [1, 2, -1]
    shards = [down_proj] + [shift(down_proj, "x", k) for k in ring]
    down_own = stacked(shards)
    down_other = swap(down_own, "c", 1)

    high = exact(norm_gain)
    mid = exact(norm_gain - high)
    low = norm_gain - high - mid
    gains = jnp.pad(jnp.stack([high, mid, low]), ((0, 5), (0, 0)))

    part = proj_parts(at, cols, proj_own, proj_other)
    near = [part[0]] + [swap(part[k], "y", k) for k in (1, 2, 3)]
    near = sum(p.astype(F32) for p in near).reshape(2, rows, 128)
    mine = jnp.arange(2)[:, None, None] == zh
    near = jnp.where(mine, near + residual.astype(F32), near).reshape(2 * rows, 128)
    far = swap(jnp.concatenate([near, gains]).astype(BF), "zh", 1).astype(F32)
    stream2 = near + far[: 2 * rows]
    other_gain = far[2 * rows : 2 * rows + 3].sum(axis=0)
    gain2 = jnp.repeat(jnp.stack(in_bits(norm_gain, other_gain, zh)), rows, axis=0)
    squares = jnp.sum((stream2 * stream2).reshape(2, rows, 128), axis=(0, 2))
    scaled2 = (stream2 * gain2).astype(BF)
    squares = jnp.pad(squares, (0, 256 - rows)).reshape(2, 128)
    high = exact(squares)
    tail = jnp.concatenate([high, squares - high, jnp.zeros((4, 128), F32)]).astype(BF)
    model = from_everyone(jnp.concatenate([scaled2, tail]), ("zp", "y"))
    squares = model[:, 2 * rows : 2 * rows + 4].astype(F32).sum(axis=0)
    squares = squares[:2] + squares[2:]

    parts = exchange(both_parts(at, model, both_own, both_other), "zq")
    squares = squares + swap(squares, "zq", 1)
    squares = squares + swap(squares, "zq", 2)
    start = 40 * zq + 8 * jnp.minimum(zq, 1)
    squares = lax.dynamic_slice_in_dim(squares.reshape(256), start, TOP, 0)
    inverse = lax.rsqrt(squares / D + 1e-05)[:, None]
    sums = parts.astype(F32).sum(axis=0)
    gate_sum, up_sum = inverse * sums[:, :ffw], inverse * sums[:, ffw:]
    hidden = (jax.nn.silu(gate_sum) * up_sum).astype(BF)
    hidden = from_everyone(hidden, "zq")
    hidden = [hidden[q, TOP - (end - begin) :] for q, begin, end in SPANS]
    hidden = jnp.concatenate(hidden)
    hidden = jnp.concatenate(in_bits(hidden, swap(hidden, "zp", 1), zp), axis=1)

    part = down_parts(at, hidden, down_own, down_other)
    near = exchange(part, "y").astype(F32).sum(axis=0).reshape(2, rows, 128)
    far = swap(pick(near, 1 - zh).astype(BF), "zh", 1)
    stream = pick(stream2.reshape(2, rows, 128), zh)
    return (stream + pick(near, zh) + far.astype(F32)).astype(BF)


def solution(mesh):
    z = mesh.shape["gz"] // 4
    split = Mesh(mesh.devices.reshape(4, 2, mesh.shape["gy"] // 2, 2, z, 4), AXES)
    gx, gz = ("x", "c"), ("zh", "y")
    in_specs = (
        P(gx, (*gz, *ZL)),
        P(gx, (*ZL, *gz)),
        P((*gz, *gx), ZL),
        P((*ZL, *gz)),
        P((*ZL, *gx), gz),
        P((*ZL, *gx), gz),
        P((*gz, *gx), ZL),
    )
    return jax.shard_map(
        on_device, mesh=split, in_specs=in_specs, out_specs=P(gx, (*ZL, *gz)), check_vma=False
    )
```

```python
import jax
import jax.numpy as jnp
from jax import lax
from jax.experimental import pallas as pl
from jax.experimental.pallas import tpu as pltpu
from jax.sharding import Mesh
from jax.sharding import PartitionSpec as P


D = 8192
BF = jnp.bfloat16
F32 = jnp.float32
AXES = ("x", "c", "zq", "zp", "zh", "y")
ZL = ("zq", "zp")
TOP = 48
STARTS_OF = (0, 48, 88, 128)
SPANS = ((0, 0, 48), (1, 48, 96), (2, 96, 136), (3, 136, 176))


def size_of(axis):
    return lax.axis_size(axis)


def shift(value, axis, step):
    n = size_of(axis)
    return lax.ppermute(value, axis, [(i, (i + step) % n) for i in range(n)])


def swap(value, axis, bit):
    n = size_of(axis)
    return lax.ppermute(value, axis, [(i, i ^ bit) for i in range(n)])


def pick(value, index, dim=0):
    return lax.dynamic_index_in_dim(value, index, dim, keepdims=False)


def exchange(parts, axis):
    return lax.all_to_all(parts, axis, split_axis=0, concat_axis=0, tiled=True)


def from_everyone(value, axis):
    copies = jnp.broadcast_to(value, (size_of(axis), *value.shape))
    return exchange(copies, axis)


def in_bits(own, other, bit):
    first = jnp.where(bit == 0, own, other)
    second = jnp.where(bit == 0, other, own)
    return first, second


def stack_kernel(*refs):
    *ins, out = refs
    height = ins[0].shape[0]
    for k, ref in enumerate(ins):
        out[k * height : (k + 1) * height] = ref[...]


def stacked(parts):
    height, width = parts[0].shape
    vmem = pl.BlockSpec(memory_space=pltpu.VMEM)
    return pl.pallas_call(
        stack_kernel,
        out_shape=jax.ShapeDtypeStruct((len(parts) * height, width), BF),
        in_specs=[vmem] * len(parts),
        out_specs=vmem,
        name="stack",
    )(*parts)


def dot(a, b):
    return jnp.dot(a, b, preferred_element_type=F32)


def proj_kernel(at, x, own, other, *outs):
    ci, zl, yi = at[0], at[2], at[3]
    rows = x.shape[1]

    def blocks(core):
        offs = [(2 * k + core) ^ zl for k in range(4)]
        return [x[((off >> 2) & 1) | (off & 2) | ((off & 1) << 2)] for off in offs]

    *outs, parts, buffer, sem = outs
    copy = pltpu.make_async_copy(other, buffer, sem)
    copy.start()
    part = dot(jnp.concatenate(blocks(ci), axis=1), own[...])
    theirs = jnp.concatenate(blocks(1 - ci), axis=1)
    copy.wait()
    part = (part + dot(theirs, buffer[...])).astype(BF)
    for zh in range(2):
        for y in range(4):
            n = (zh * 4 + y) * 128
            parts[y, zh * rows : (zh + 1) * rows] = part[:, n : n + 128]
    for k, out in enumerate(outs):
        out[...] = parts[yi ^ k]


def proj_parts(at, x, own, other):
    rows = x.shape[1]
    vmem, hbm = pl.BlockSpec(memory_space=pltpu.VMEM), pl.BlockSpec(memory_space=pltpu.HBM)
    return pl.pallas_call(
        proj_kernel,
        out_shape=[jax.ShapeDtypeStruct((2 * rows, 128), BF)] * 4,
        in_specs=[pl.BlockSpec(memory_space=pltpu.SMEM), vmem, vmem, hbm],
        out_specs=[vmem] * 4,
        scratch_shapes=[
            pltpu.VMEM((4, 2 * rows, 128), BF),
            pltpu.VMEM(other.shape, BF),
            pltpu.SemaphoreType.DMA(()),
        ],
        cost_estimate=pl.CostEstimate(
            flops=2 * rows * 1024 * 1024, bytes_accessed=3 << 20, transcendentals=0
        ),
        name="proj_mm",
    )(at, x, own, other)


def both_kernel(at, x, own, other, out):
    ci, zp = at[0], at[1]
    rows = (x.shape[1] - 8) // 2

    def blocks(core):
        parts = []
        for k in range(4):
            for turn in range(2):
                at_block = (zp ^ turn) * 4 + (k % 2) * 2 + core
                parts.append(x[at_block, pl.ds((k // 2) * rows, rows)])
        return jnp.concatenate(parts, axis=1)

    part = (dot(blocks(ci), own[...]) + dot(blocks(1 - ci), other[...])).astype(BF)
    for q in range(4):
        out[q] = part[STARTS_OF[q] : STARTS_OF[q] + TOP]

    @pl.when(pl.program_id(0) == pl.num_programs(0) - 1)
    def _():
        squares = sum(x[k, pl.ds(2 * rows, 4)].astype(F32) for k in range(8))
        squares = jnp.concatenate([squares[k : k + 1] + squares[k + 2 : k + 3] for k in (0, 1)], 1)
        lane = lax.broadcasted_iota(jnp.int32, (TOP, 256), 1)
        row = lax.broadcasted_iota(jnp.int32, (TOP, 256), 0)
        for q in range(4):
            own_lane = jnp.where(lane == row + STARTS_OF[q], squares, 0.0)
            total = jnp.sum(own_lane, axis=1, keepdims=True)
            high = total.astype(BF).astype(F32)
            place = lane[:, :128]
            tail = jnp.where(place == 0, high, jnp.where(place == 1, total - high, 0.0))
            out[q, :, out.shape[2] - 128 :] = tail.astype(BF)


def both_parts(at, x, own, other):
    depth, wide = own.shape
    tile = (wide + 128) // 3
    vmem = pl.BlockSpec(memory_space=pltpu.VMEM)
    weights = pl.BlockSpec((depth, tile), lambda n: (0, n))
    return pl.pallas_call(
        both_kernel,
        grid=(3,),
        out_shape=jax.ShapeDtypeStruct((4, TOP, 3 * tile), BF),
        in_specs=[pl.BlockSpec(memory_space=pltpu.SMEM), vmem, weights, weights],
        out_specs=pl.BlockSpec((4, TOP, tile), lambda n: (0, 0, n)),
        cost_estimate=pl.CostEstimate(
            flops=4 * 176 * depth * wide, bytes_accessed=9 << 20, transcendentals=0
        ),
        name="both_mm",
    )(at, x, own, other)


def down_kernel(at, near, far, own, other, out, whole, sems):
    ci, zp, xi = at[0], at[1], at[4]
    height = own.shape[0] // 4
    half = near.shape[1]

    def place(k, core):
        b = ((xi + 4 - k) & 3) * 2 + core
        return pl.ds(pl.multiple_of(b * height, 16), height)

    copies = []
    for k in range(4):
        source = other.at[pl.ds(k * height, height)]
        copies.append(pltpu.make_async_copy(source, whole.at[place(k, 1 - ci)], sems.at[k]))
        copies[k].start()
    for k in range(4):
        whole[place(k, ci)] = own[k * height : (k + 1) * height]
    for copy in copies:
        copy.wait()
    part = dot(near[...], whole[pl.ds(pl.multiple_of(zp * half, 16), half)])
    part = part + dot(far[...], whole[pl.ds(pl.multiple_of((1 - zp) * half, 16), half)])
    for n in range(8):
        out[n] = part[:, n * 128 : (n + 1) * 128].astype(BF)


def down_parts(at, near, far, own, other):
    rows, half = near.shape
    vmem, hbm = pl.BlockSpec(memory_space=pltpu.VMEM), pl.BlockSpec(memory_space=pltpu.HBM)
    return pl.pallas_call(
        down_kernel,
        out_shape=jax.ShapeDtypeStruct((8, rows, 128), BF),
        in_specs=[pl.BlockSpec(memory_space=pltpu.SMEM), vmem, vmem, vmem, hbm],
        out_specs=vmem,
        scratch_shapes=[pltpu.VMEM((2 * half, 1024), BF), pltpu.SemaphoreType.DMA((4,))],
        cost_estimate=pl.CostEstimate(
            flops=4 * rows * half * 1024, bytes_accessed=5 << 20, transcendentals=0
        ),
        name="down_mm",
    )(at, near, far, own, other)


def exact(value):
    return lax.reduce_precision(value, 8, 7)


def on_device(attn_out, residual, proj_weight, norm_gain, gate_proj, up_proj, down_proj):
    xi, ci, zh, yi = (lax.axis_index(name) for name in ("x", "c", "zh", "y"))
    zq, zp = lax.axis_index("zq"), lax.axis_index("zp")
    at = jnp.stack([ci, zp, 2 * zq + zp, yi, xi]).astype(jnp.int32)
    rows = attn_out.shape[0]
    ffw = gate_proj.shape[1] // 2

    cols = attn_out[None]
    for bit in (4, 2, 1):
        cols = jnp.concatenate([cols, swap(cols, ZL, bit)])

    def columns(which):
        halves = [lax.dynamic_slice_in_dim(w, which * ffw, ffw, 1) for w in (gate_proj, up_proj)]
        return jnp.concatenate(halves, axis=1)

    facing = swap(columns(1 - zp), "zp", 1)
    both = jnp.concatenate([columns(zp), facing])
    both_own = from_everyone(both, "x").reshape(-1, 2 * ffw)
    both_other = swap(both_own, "c", 1)
    proj_own = from_everyone(proj_weight, "x").reshape(-1, proj_weight.shape[1])
    proj_other = swap(proj_own, "c", 1)
    ring = [1, 2, -1]
    shards = [down_proj] + [shift(down_proj, "x", k) for k in ring]
    down_own = stacked(shards)
    down_other = swap(down_own, "c", 1)

    high = exact(norm_gain)
    mid = exact(norm_gain - high)
    low = norm_gain - high - mid
    gains = jnp.pad(jnp.stack([high, mid, low]), ((0, 5), (0, 0)))

    part = proj_parts(at, cols, proj_own, proj_other)
    near = [part[0]] + [swap(part[k], "y", k) for k in (1, 2, 3)]
    near = sum(p.astype(F32) for p in near).reshape(2, rows, 128)
    mine = jnp.arange(2)[:, None, None] == zh
    near = jnp.where(mine, near + residual.astype(F32), near).reshape(2 * rows, 128)
    far = swap(jnp.concatenate([near, gains]).astype(BF), "zh", 1).astype(F32)
    stream2 = near + far[: 2 * rows]
    other_gain = far[2 * rows : 2 * rows + 3].sum(axis=0)
    gain2 = jnp.repeat(jnp.stack(in_bits(norm_gain, other_gain, zh)), rows, axis=0)
    squares = jnp.sum((stream2 * stream2).reshape(2, rows, 128), axis=(0, 2))
    scaled2 = (stream2 * gain2).astype(BF)
    squares = jnp.pad(squares, (0, 256 - rows)).reshape(2, 128)
    high = exact(squares)
    tail = jnp.concatenate([high, squares - high, jnp.zeros((4, 128), F32)]).astype(BF)
    model = from_everyone(jnp.concatenate([scaled2, tail]), ("zp", "y"))
    parts = exchange(both_parts(at, model, both_own, both_other), "zq")
    sums = parts.astype(F32).sum(axis=0)
    squares = sums[:, 2 * ffw] + sums[:, 2 * ffw + 1]
    inverse = lax.rsqrt(squares / D + 1e-05)[:, None]
    gate_sum, up_sum = inverse * sums[:, :ffw], inverse * sums[:, ffw : 2 * ffw]
    hidden = (jax.nn.silu(gate_sum) * up_sum).astype(BF)
    hidden = from_everyone(hidden, "zq")
    hidden = [hidden[q, TOP - (end - begin) :] for q, begin, end in SPANS]
    hidden = jnp.concatenate(hidden)
    facing = swap(hidden, "zp", 1)

    part = down_parts(at, hidden, facing, down_own, down_other)
    down_sum = exchange(part, ("zh", "y")).astype(F32).sum(axis=0)
    stream = pick(stream2.reshape(2, rows, 128), zh)
    return (stream + down_sum).astype(BF)


def solution(mesh):
    z = mesh.shape["gz"] // 4
    split = Mesh(mesh.devices.reshape(4, 2, mesh.shape["gy"] // 2, 2, z, 4), AXES)
    gx, gz = ("x", "c"), ("zh", "y")
    in_specs = (
        P(gx, (*gz, *ZL)),
        P(gx, (*ZL, *gz)),
        P((*gz, *gx), ZL),
        P((*ZL, *gz)),
        P((*ZL, *gx), gz),
        P((*ZL, *gx), gz),
        P((*gz, *gx), ZL),
    )
    return jax.shard_map(
        on_device, mesh=split, in_specs=in_specs, out_specs=P(gx, (*ZL, *gz)), check_vma=False
    )
```

```python
import jax
import jax.numpy as jnp
from jax import lax
from jax.experimental import pallas as pl
from jax.experimental.pallas import tpu as pltpu
from jax.sharding import Mesh
from jax.sharding import PartitionSpec as P


D = 8192
BF = jnp.bfloat16
F32 = jnp.float32
AXES = ("x", "c", "zq", "zp", "zh", "y")
ZL = ("zq", "zp")
TOP = 48


def size_of(axis):
    return lax.axis_size(axis)


def shift(value, axis, step):
    n = size_of(axis)
    return lax.ppermute(value, axis, [(i, (i + step) % n) for i in range(n)])


def swap(value, axis, bit):
    n = size_of(axis)
    return lax.ppermute(value, axis, [(i, i ^ bit) for i in range(n)])


def pick(value, index, dim=0):
    return lax.dynamic_index_in_dim(value, index, dim, keepdims=False)


def exchange(parts, axis):
    return lax.all_to_all(parts, axis, split_axis=0, concat_axis=0, tiled=True)


def from_everyone(value, axis):
    copies = jnp.broadcast_to(value, (size_of(axis), *value.shape))
    return exchange(copies, axis)


def in_bits(own, other, bit):
    first = jnp.where(bit == 0, own, other)
    second = jnp.where(bit == 0, other, own)
    return first, second


def stack_kernel(*refs):
    *ins, out = refs
    height = ins[0].shape[0]
    for k, ref in enumerate(ins):
        out[k * height : (k + 1) * height] = ref[...]


def stacked(parts):
    height, width = parts[0].shape
    vmem = pl.BlockSpec(memory_space=pltpu.VMEM)
    return pl.pallas_call(
        stack_kernel,
        out_shape=jax.ShapeDtypeStruct((len(parts) * height, width), BF),
        in_specs=[vmem] * len(parts),
        out_specs=vmem,
        name="stack",
    )(*parts)


def dot(a, b):
    return jnp.dot(a, b, preferred_element_type=F32)


def proj_kernel(at, x, own, other, *outs):
    ci, zl, yi = at[0], at[2], at[3]
    rows = x.shape[1]

    def blocks(core):
        offs = [(2 * k + core) ^ zl for k in range(4)]
        return [x[((off >> 2) & 1) | (off & 2) | ((off & 1) << 2)] for off in offs]

    mine = jnp.concatenate(blocks(ci), axis=1)
    theirs = jnp.concatenate(blocks(1 - ci), axis=1)
    part = (dot(mine, own[...]) + dot(theirs, other[...])).astype(BF)
    *outs, parts = outs
    for zh in range(2):
        for y in range(4):
            n = (zh * 4 + y) * 128
            parts[y, zh * rows : (zh + 1) * rows] = part[:, n : n + 128]
    for k, out in enumerate(outs):
        out[...] = parts[yi ^ k]


def proj_parts(at, x, own, other):
    rows = x.shape[1]
    vmem = pl.BlockSpec(memory_space=pltpu.VMEM)
    return pl.pallas_call(
        proj_kernel,
        out_shape=[jax.ShapeDtypeStruct((2 * rows, 128), BF)] * 4,
        in_specs=[pl.BlockSpec(memory_space=pltpu.SMEM), vmem, vmem, vmem],
        out_specs=[vmem] * 4,
        scratch_shapes=[pltpu.VMEM((4, 2 * rows, 128), BF)],
        cost_estimate=pl.CostEstimate(
            flops=2 * rows * 1024 * 1024, bytes_accessed=3 << 20, transcendentals=0
        ),
        name="proj_mm",
    )(at, x, own, other)


def both_kernel(at, x, own, other, send, keep):
    ci, zp, bit = at[0], at[1], (at[2] >> 1) & 1
    rows = (x.shape[1] - 8) // 2

    def blocks(core):
        parts = []
        for k in range(4):
            for turn in range(2):
                at_block = (zp ^ turn) * 4 + (k % 2) * 2 + core
                parts.append(x[at_block, pl.ds((k // 2) * rows, rows)])
        return jnp.concatenate(parts, axis=1)

    part = dot(blocks(ci), own[...]) + dot(blocks(1 - ci), other[...])
    upper, lower = part[: rows // 2], part[rows // 2 :]
    send[...] = jnp.where(bit == 0, lower, upper).astype(BF)
    keep[...] = jnp.where(bit == 0, upper, lower)


def both_parts(at, x, own, other, half):
    depth, wide = own.shape
    tile = wide // 2
    vmem = pl.BlockSpec(memory_space=pltpu.VMEM)
    weights = pl.BlockSpec((depth, tile), lambda n: (0, n))
    result = pl.BlockSpec((half, tile), lambda n: (0, n))
    return pl.pallas_call(
        both_kernel,
        grid=(2,),
        out_shape=[jax.ShapeDtypeStruct((half, wide), kind) for kind in (BF, F32)],
        in_specs=[pl.BlockSpec(memory_space=pltpu.SMEM), vmem, weights, weights],
        out_specs=[result, result],
        cost_estimate=pl.CostEstimate(
            flops=8 * half * depth * wide, bytes_accessed=9 << 20, transcendentals=0
        ),
        name="both_mm",
    )(at, x, own, other)


def near_kernel(at, x, own, other, part, rest, whole):
    ci, zp, xi = at[0], at[1], at[4]
    height = own.shape[0] // 4
    half = x.shape[1]
    for ref, core in ((own, ci), (other, 1 - ci)):
        for k in range(4):
            b = ((xi + 4 - k) & 3) * 2 + core
            to = pl.ds(pl.multiple_of(b * height, 16), height)
            whole[to] = ref[k * height : (k + 1) * height]
    part[...] = dot(x[...], whole[pl.ds(pl.multiple_of(zp * half, 16), half)])
    rest[...] = whole[pl.ds(pl.multiple_of((1 - zp) * half, 16), half)]


def far_kernel(x, part, rest, out):
    rows = x.shape[0]
    total = (part[...] + dot(x[...], rest[...])).astype(BF)
    for zh in range(2):
        for y in range(4):
            n = (zh * 4 + y) * 128
            out[y, zh * rows : (zh + 1) * rows] = total[:, n : n + 128]


def near_part(at, x, own, other):
    rows, half = x.shape
    wide = own.shape[1]
    vmem = pl.BlockSpec(memory_space=pltpu.VMEM)
    return pl.pallas_call(
        near_kernel,
        out_shape=(
            jax.ShapeDtypeStruct((rows, wide), F32),
            jax.ShapeDtypeStruct((half, wide), BF),
        ),
        in_specs=[pl.BlockSpec(memory_space=pltpu.SMEM), vmem, vmem, vmem],
        out_specs=(vmem, vmem),
        scratch_shapes=[pltpu.VMEM((2 * half, wide), BF)],
        cost_estimate=pl.CostEstimate(
            flops=2 * rows * half * wide, bytes_accessed=5 << 20, transcendentals=0
        ),
        name="near_mm",
    )(at, x, own, other)


def down_parts(x, part, rest):
    rows, half = x.shape
    vmem = pl.BlockSpec(memory_space=pltpu.VMEM)
    return pl.pallas_call(
        far_kernel,
        out_shape=jax.ShapeDtypeStruct((4, 2 * rows, 128), BF),
        in_specs=[vmem, vmem, vmem],
        out_specs=vmem,
        cost_estimate=pl.CostEstimate(
            flops=2 * rows * half * 1024, bytes_accessed=3 << 20, transcendentals=0
        ),
        name="far_mm",
    )(x, part, rest)


def exact(value):
    return lax.reduce_precision(value, 8, 7)


def on_device(attn_out, residual, proj_weight, norm_gain, gate_proj, up_proj, down_proj):
    xi, ci, zh, yi = (lax.axis_index(name) for name in ("x", "c", "zh", "y"))
    zq, zp = lax.axis_index("zq"), lax.axis_index("zp")
    at = jnp.stack([ci, zp, 2 * zq + zp, yi, xi]).astype(jnp.int32)
    rows = attn_out.shape[0]
    ffw = gate_proj.shape[1] // 2

    cols = attn_out[None]
    for bit in (4, 2, 1):
        cols = jnp.concatenate([cols, swap(cols, ZL, bit)])

    def columns(which):
        halves = [lax.dynamic_slice_in_dim(w, which * ffw, ffw, 1) for w in (gate_proj, up_proj)]
        return jnp.concatenate(halves, axis=1)

    facing = swap(columns(1 - zp), "zp", 1)
    both = jnp.concatenate([columns(zp), facing])
    both_own = from_everyone(both, "x").reshape(-1, 2 * ffw)
    both_other = swap(both_own, "c", 1)
    proj_own = from_everyone(proj_weight, "x").reshape(-1, proj_weight.shape[1])
    proj_other = swap(proj_own, "c", 1)
    ring = [1, 2, -1]
    shards = [down_proj] + [shift(down_proj, "x", k) for k in ring]
    down_own = stacked(shards)
    down_other = swap(down_own, "c", 1)

    high = exact(norm_gain)
    mid = exact(norm_gain - high)
    low = norm_gain - high - mid
    gains = jnp.pad(jnp.stack([high, mid, low]), ((0, 5), (0, 0)))

    part = proj_parts(at, cols, proj_own, proj_other)
    near = [part[0]] + [swap(part[k], "y", k) for k in (1, 2, 3)]
    near = sum(p.astype(F32) for p in near).reshape(2, rows, 128)
    mine = jnp.arange(2)[:, None, None] == zh
    near = jnp.where(mine, near + residual.astype(F32), near).reshape(2 * rows, 128)
    far = swap(jnp.concatenate([near, gains]).astype(BF), "zh", 1).astype(F32)
    stream2 = near + far[: 2 * rows]
    other_gain = far[2 * rows : 2 * rows + 3].sum(axis=0)
    gain2 = jnp.repeat(jnp.stack(in_bits(norm_gain, other_gain, zh)), rows, axis=0)
    squares = jnp.sum((stream2 * stream2).reshape(2, rows, 128), axis=(0, 2))
    scaled2 = (stream2 * gain2).astype(BF)
    squares = jnp.pad(squares, (0, 256 - rows)).reshape(2, 128)
    high = exact(squares)
    tail = jnp.concatenate([high, squares - high, jnp.zeros((4, 128), F32)]).astype(BF)
    model = from_everyone(jnp.concatenate([scaled2, tail]), ("zp", "y"))
    squares = model[:, 2 * rows : 2 * rows + 4].astype(F32).sum(axis=0)
    squares = squares[:2] + squares[2:]

    half, step = rows // 2, rows // 2 - TOP
    bit1, bit2 = zq & 1, zq >> 1
    send, keep = both_parts(at, model, both_own, both_other, half)
    got = swap(send, "zq", 1)
    squares = squares + swap(squares, "zq", 1)
    sums = keep + got.astype(F32)
    sent = lax.dynamic_slice_in_dim(sums, step * (1 - bit2), TOP, 0).astype(BF)
    got = swap(sent, "zq", 2)
    squares = squares + swap(squares, "zq", 2)
    sums = lax.dynamic_slice_in_dim(sums, step * bit2, TOP, 0) + got.astype(F32)
    squares = lax.dynamic_slice_in_dim(squares.reshape(256), half * bit1 + step * bit2, TOP, 0)
    inverse = lax.rsqrt(squares / D + 1e-05)[:, None]
    gate_sum, up_sum = inverse * sums[:, :ffw], inverse * sums[:, ffw:]
    hidden = (jax.nn.silu(gate_sum) * up_sum).astype(BF)
    upper, lower = in_bits(hidden, swap(hidden, "zq", 2), bit2)
    hidden = jnp.concatenate([upper, lower[2 * TOP - half :]])
    hidden = jnp.concatenate(in_bits(hidden, swap(hidden, "zq", 1), bit1))
    hidden, down_other = lax.optimization_barrier((hidden, down_other))
    facing = swap(hidden, "zp", 1)

    part, rest = near_part(at, hidden, down_own, down_other)
    part = down_parts(facing, part, rest)
    near = exchange(part, "y").astype(F32).sum(axis=0).reshape(2, rows, 128)
    far = swap(pick(near, 1 - zh).astype(BF), "zh", 1)
    stream = pick(stream2.reshape(2, rows, 128), zh)
    return (stream + pick(near, zh) + far.astype(F32)).astype(BF)


def solution(mesh):
    z = mesh.shape["gz"] // 4
    split = Mesh(mesh.devices.reshape(4, 2, mesh.shape["gy"] // 2, 2, z, 4), AXES)
    gx, gz = ("x", "c"), ("zh", "y")
    in_specs = (
        P(gx, (*gz, *ZL)),
        P(gx, (*ZL, *gz)),
        P((*gz, *gx), ZL),
        P((*ZL, *gz)),
        P((*ZL, *gx), gz),
        P((*ZL, *gx), gz),
        P((*gz, *gx), ZL),
    )
    return jax.shard_map(
        on_device, mesh=split, in_specs=in_specs, out_specs=P(gx, (*ZL, *gz)), check_vma=False
    )
```

```python
import jax
import jax.numpy as jnp
from jax import lax
from jax.experimental import pallas as pl
from jax.experimental.pallas import tpu as pltpu
from jax.sharding import Mesh
from jax.sharding import PartitionSpec as P


D = 8192
BF = jnp.bfloat16
F32 = jnp.float32
AXES = ("x", "c", "zq", "zp", "zh", "y")
ZL = ("zq", "zp")
TOP = 48


def size_of(axis):
    return lax.axis_size(axis)


def swap(value, axis, bit):
    n = size_of(axis)
    return lax.ppermute(value, axis, [(i, i ^ bit) for i in range(n)])


def pick(value, index, dim=0):
    return lax.dynamic_index_in_dim(value, index, dim, keepdims=False)


def exchange(parts, axis):
    return lax.all_to_all(parts, axis, split_axis=0, concat_axis=0, tiled=True)


def from_everyone(value, axis):
    copies = jnp.broadcast_to(value, (size_of(axis), *value.shape))
    return exchange(copies, axis)


def in_bits(own, other, bit):
    first = jnp.where(bit == 0, own, other)
    second = jnp.where(bit == 0, other, own)
    return first, second


def gathered(w):
    own = lax.all_gather(w, "x", axis=0, tiled=True)
    return own, swap(own, "c", 1)


def dot(a, b):
    return jnp.dot(a, b, preferred_element_type=F32)


def proj_kernel(at, x, own, other, out):
    ci, zl = at[0], at[2]
    rows = x.shape[1]

    def blocks(core):
        offs = [(2 * k + core) ^ zl for k in range(4)]
        return [x[((off >> 2) & 1) | (off & 2) | ((off & 1) << 2)] for off in offs]

    mine = jnp.concatenate(blocks(ci), axis=1)
    theirs = jnp.concatenate(blocks(1 - ci), axis=1)
    part = (dot(mine, own[...]) + dot(theirs, other[...])).astype(BF)
    for zh in range(2):
        for y in range(4):
            n = (zh * 4 + y) * 128
            out[y, zh * rows : (zh + 1) * rows] = part[:, n : n + 128]


def proj_parts(at, x, own, other):
    rows = x.shape[1]
    vmem = pl.BlockSpec(memory_space=pltpu.VMEM)
    return pl.pallas_call(
        proj_kernel,
        out_shape=jax.ShapeDtypeStruct((4, 2 * rows, 128), BF),
        in_specs=[pl.BlockSpec(memory_space=pltpu.SMEM), vmem, vmem, vmem],
        out_specs=vmem,
        cost_estimate=pl.CostEstimate(
            flops=2 * rows * 1024 * 1024, bytes_accessed=3 << 20, transcendentals=0
        ),
        name="proj_mm",
    )(at, x, own, other)


def both_kernel(at, x, own, other, send, keep):
    ci, zp, bit = at[0], at[1], (at[2] >> 1) & 1
    rows = (x.shape[1] - 8) // 2

    def blocks(core):
        parts = []
        for k in range(4):
            for turn in range(2):
                at_block = (zp ^ turn) * 4 + (k % 2) * 2 + core
                parts.append(x[at_block, pl.ds((k // 2) * rows, rows)])
        return jnp.concatenate(parts, axis=1)

    part = dot(blocks(ci), own[...]) + dot(blocks(1 - ci), other[...])
    upper, lower = part[: rows // 2], part[rows // 2 :]
    send[...] = jnp.where(bit == 0, lower, upper).astype(BF)
    keep[...] = jnp.where(bit == 0, upper, lower)


def both_parts(at, x, own, other, half):
    depth, wide = own.shape
    tile = wide // 2
    vmem = pl.BlockSpec(memory_space=pltpu.VMEM)
    weights = pl.BlockSpec((depth, tile), lambda n: (0, n))
    result = pl.BlockSpec((half, tile), lambda n: (0, n))
    return pl.pallas_call(
        both_kernel,
        grid=(2,),
        out_shape=[jax.ShapeDtypeStruct((half, wide), kind) for kind in (BF, F32)],
        in_specs=[pl.BlockSpec(memory_space=pltpu.SMEM), vmem, weights, weights],
        out_specs=[result, result],
        cost_estimate=pl.CostEstimate(
            flops=8 * half * depth * wide, bytes_accessed=9 << 20, transcendentals=0
        ),
        name="both_mm",
    )(at, x, own, other)


def near_kernel(at, x, own, other, part, rest, whole):
    ci, zp = at[0], at[1]
    height = own.shape[0] // 4
    half = x.shape[1]
    for ref, core in ((own, ci), (other, 1 - ci)):
        for k in range(4):
            b = 2 * k + core
            to = pl.ds(pl.multiple_of(b * height, 16), height)
            whole[to] = ref[k * height : (k + 1) * height]
    part[...] = dot(x[...], whole[pl.ds(pl.multiple_of(zp * half, 16), half)])
    rest[...] = whole[pl.ds(pl.multiple_of((1 - zp) * half, 16), half)]


def far_kernel(x, part, rest, out):
    rows = x.shape[0]
    total = (part[...] + dot(x[...], rest[...])).astype(BF)
    for zh in range(2):
        for y in range(4):
            n = (zh * 4 + y) * 128
            out[y, zh * rows : (zh + 1) * rows] = total[:, n : n + 128]


def near_part(at, x, own, other):
    rows, half = x.shape
    wide = own.shape[1]
    vmem = pl.BlockSpec(memory_space=pltpu.VMEM)
    return pl.pallas_call(
        near_kernel,
        out_shape=(
            jax.ShapeDtypeStruct((rows, wide), F32),
            jax.ShapeDtypeStruct((half, wide), BF),
        ),
        in_specs=[pl.BlockSpec(memory_space=pltpu.SMEM), vmem, vmem, vmem],
        out_specs=(vmem, vmem),
        scratch_shapes=[pltpu.VMEM((2 * half, wide), BF)],
        cost_estimate=pl.CostEstimate(
            flops=2 * rows * half * wide, bytes_accessed=5 << 20, transcendentals=0
        ),
        name="near_mm",
    )(at, x, own, other)


def down_parts(x, part, rest):
    rows, half = x.shape
    vmem = pl.BlockSpec(memory_space=pltpu.VMEM)
    return pl.pallas_call(
        far_kernel,
        out_shape=jax.ShapeDtypeStruct((4, 2 * rows, 128), BF),
        in_specs=[vmem, vmem, vmem],
        out_specs=vmem,
        cost_estimate=pl.CostEstimate(
            flops=2 * rows * half * 1024, bytes_accessed=3 << 20, transcendentals=0
        ),
        name="far_mm",
    )(x, part, rest)


def exact(value):
    return lax.reduce_precision(value, 8, 7)


def on_device(attn_out, residual, proj_weight, norm_gain, gate_proj, up_proj, down_proj):
    ci, zh = lax.axis_index("c"), lax.axis_index("zh")
    zq, zp = lax.axis_index("zq"), lax.axis_index("zp")
    at = jnp.stack([ci, zp, 2 * zq + zp]).astype(jnp.int32)
    rows = attn_out.shape[0]
    ffw = gate_proj.shape[1] // 2

    cols = attn_out[None]
    for bit in (4, 2, 1):
        arrived = swap(cols, ZL, bit)
        cols = jnp.concatenate([cols, arrived])

    def columns(which):
        halves = [lax.dynamic_slice_in_dim(w, which * ffw, ffw, 1) for w in (gate_proj, up_proj)]
        return jnp.concatenate(halves, axis=1)

    facing = swap(columns(1 - zp), "zp", 1)
    both = jnp.concatenate([columns(zp), facing])
    proj_own, proj_other = gathered(proj_weight)
    both_own, both_other = gathered(both)
    down_own, down_other = gathered(down_proj)

    high = exact(norm_gain)
    mid = exact(norm_gain - high)
    low = norm_gain - high - mid
    gains = jnp.pad(jnp.stack([high, mid, low]), ((0, 5), (0, 0)))

    part = proj_parts(at, cols, proj_own, proj_other)
    near = exchange(part, "y").astype(F32).sum(axis=0).reshape(2, rows, 128)
    mine = jnp.arange(2)[:, None, None] == zh
    near = jnp.where(mine, near + residual.astype(F32), near).reshape(2 * rows, 128)
    far = swap(jnp.concatenate([near, gains]).astype(BF), "zh", 1).astype(F32)
    stream2 = near + far[: 2 * rows]
    other_gain = far[2 * rows : 2 * rows + 3].sum(axis=0)
    gain2 = jnp.repeat(jnp.stack(in_bits(norm_gain, other_gain, zh)), rows, axis=0)
    squares = jnp.sum((stream2 * stream2).reshape(2, rows, 128), axis=(0, 2))
    scaled2 = (stream2 * gain2).astype(BF)
    squares = jnp.pad(squares, (0, 256 - rows)).reshape(2, 128)
    high = exact(squares)
    tail = jnp.concatenate([high, squares - high, jnp.zeros((4, 128), F32)]).astype(BF)
    model = from_everyone(jnp.concatenate([scaled2, tail]), ("zp", "y"))
    squares = model[:, 2 * rows : 2 * rows + 4].astype(F32).sum(axis=0)
    squares = squares[:2] + squares[2:]

    half, step = rows // 2, rows // 2 - TOP
    bit1, bit2 = zq & 1, zq >> 1
    send, keep = both_parts(at, model, both_own, both_other, half)
    got = swap(send, "zq", 1)
    squares = squares + swap(squares, "zq", 1)
    sums = keep + got.astype(F32)
    sent = lax.dynamic_slice_in_dim(sums, step * (1 - bit2), TOP, 0).astype(BF)
    got = swap(sent, "zq", 2)
    squares = squares + swap(squares, "zq", 2)
    sums = lax.dynamic_slice_in_dim(sums, step * bit2, TOP, 0) + got.astype(F32)
    squares = lax.dynamic_slice_in_dim(squares.reshape(256), half * bit1 + step * bit2, TOP, 0)
    inverse = lax.rsqrt(squares / D + 1e-05)[:, None]
    gate_sum, up_sum = inverse * sums[:, :ffw], inverse * sums[:, ffw:]
    hidden = (jax.nn.silu(gate_sum) * up_sum).astype(BF)
    upper, lower = in_bits(hidden, swap(hidden, "zq", 2), bit2)
    hidden = jnp.concatenate([upper, lower[2 * TOP - half :]])
    hidden = jnp.concatenate(in_bits(hidden, swap(hidden, "zq", 1), bit1))
    hidden, down_other = lax.optimization_barrier((hidden, down_other))
    facing = swap(hidden, "zp", 1)

    part, rest = near_part(at, hidden, down_own, down_other)
    part = down_parts(facing, part, rest)
    near = exchange(part, "y").astype(F32).sum(axis=0).reshape(2, rows, 128)
    far = swap(pick(near, 1 - zh).astype(BF), "zh", 1)
    stream = pick(stream2.reshape(2, rows, 128), zh)
    return (stream + pick(near, zh) + far.astype(F32)).astype(BF)


def solution(mesh):
    z = mesh.shape["gz"] // 4
    split = Mesh(mesh.devices.reshape(4, 2, mesh.shape["gy"] // 2, 2, z, 4), AXES)
    gx, gz = ("x", "c"), ("zh", "y")
    in_specs = (
        P(gx, (*gz, *ZL)),
        P(gx, (*ZL, *gz)),
        P((*gz, *gx), ZL),
        P((*ZL, *gz)),
        P((*ZL, *gx), gz),
        P((*ZL, *gx), gz),
        P((*gz, *gx), ZL),
    )
    return jax.shard_map(
        on_device, mesh=split, in_specs=in_specs, out_specs=P(gx, (*ZL, *gz)), check_vma=False
    )
```

```python
import jax
import jax.numpy as jnp
from jax import lax
from jax.experimental import pallas as pl
from jax.experimental.pallas import tpu as pltpu
from jax.sharding import Mesh
from jax.sharding import PartitionSpec as P


D = 8192
BF = jnp.bfloat16
F32 = jnp.float32
AXES = ("x", "c", "zq", "zp", "zh", "y")
ZL = ("zq", "zp")
TOP = 48


def size_of(axis):
    return lax.axis_size(axis)


def shift(value, axis, step):
    n = size_of(axis)
    return lax.ppermute(value, axis, [(i, (i + step) % n) for i in range(n)])


def swap(value, axis, bit):
    n = size_of(axis)
    return lax.ppermute(value, axis, [(i, i ^ bit) for i in range(n)])


def pick(value, index, dim=0):
    return lax.dynamic_index_in_dim(value, index, dim, keepdims=False)


def exchange(parts, axis):
    return lax.all_to_all(parts, axis, split_axis=0, concat_axis=0, tiled=True)


def from_everyone(value, axis):
    copies = jnp.broadcast_to(value, (size_of(axis), *value.shape))
    return exchange(copies, axis)


def in_bits(own, other, bit):
    first = jnp.where(bit == 0, own, other)
    second = jnp.where(bit == 0, other, own)
    return first, second


def stack_kernel(*refs):
    *ins, out = refs
    height = ins[0].shape[0]
    for k, ref in enumerate(ins):
        out[k * height : (k + 1) * height] = ref[...]


def stacked(parts):
    height, width = parts[0].shape
    vmem = pl.BlockSpec(memory_space=pltpu.VMEM)
    return pl.pallas_call(
        stack_kernel,
        out_shape=jax.ShapeDtypeStruct((len(parts) * height, width), BF),
        in_specs=[vmem] * len(parts),
        out_specs=vmem,
        name="stack",
    )(*parts)


def ring_gathered(w):
    ring = [1, 2, -1]
    shards = [w] + [shift(w, "x", k) for k in ring]
    own = stacked(shards)
    return own, swap(own, "c", 1)


def dot(a, b):
    return jnp.dot(a, b, preferred_element_type=F32)


def proj_kernel(at, x, own, other, out):
    ci, zl = at[0], at[2]
    rows = x.shape[1]

    def blocks(core):
        offs = [(2 * k + core) ^ zl for k in range(4)]
        return [x[((off >> 2) & 1) | (off & 2) | ((off & 1) << 2)] for off in offs]

    mine = jnp.concatenate(blocks(ci), axis=1)
    theirs = jnp.concatenate(blocks(1 - ci), axis=1)
    part = (dot(mine, own[...]) + dot(theirs, other[...])).astype(BF)
    for zh in range(2):
        for y in range(4):
            n = (zh * 4 + y) * 128
            out[y, zh * rows : (zh + 1) * rows] = part[:, n : n + 128]


def proj_parts(at, x, own, other):
    rows = x.shape[1]
    vmem = pl.BlockSpec(memory_space=pltpu.VMEM)
    return pl.pallas_call(
        proj_kernel,
        out_shape=jax.ShapeDtypeStruct((4, 2 * rows, 128), BF),
        in_specs=[pl.BlockSpec(memory_space=pltpu.SMEM), vmem, vmem, vmem],
        out_specs=vmem,
        cost_estimate=pl.CostEstimate(
            flops=2 * rows * 1024 * 1024, bytes_accessed=3 << 20, transcendentals=0
        ),
        name="proj_mm",
    )(at, x, own, other)


def both_kernel(at, x, own, other, send, keep):
    ci, zp, bit, xi = at[0], at[1], (at[2] >> 1) & 1, at[3]
    rows = (x.shape[1] - 8) // 2

    def blocks(core):
        parts = []
        for k in range(4):
            place = (xi + 4 - k) & 3
            row = pl.multiple_of((place >> 1) * rows, 16)
            for turn in range(2):
                at_block = (zp ^ turn) * 4 + (place & 1) * 2 + core
                parts.append(x[at_block, pl.ds(row, rows)])
        return jnp.concatenate(parts, axis=1)

    part = dot(blocks(ci), own[...]) + dot(blocks(1 - ci), other[...])
    upper, lower = part[: rows // 2], part[rows // 2 :]
    send[...] = jnp.where(bit == 0, lower, upper).astype(BF)
    keep[...] = jnp.where(bit == 0, upper, lower)


def both_parts(at, x, own, other, half):
    depth, wide = own.shape
    tile = wide // 2
    vmem = pl.BlockSpec(memory_space=pltpu.VMEM)
    weights = pl.BlockSpec((depth, tile), lambda n: (0, n))
    result = pl.BlockSpec((half, tile), lambda n: (0, n))
    return pl.pallas_call(
        both_kernel,
        grid=(2,),
        out_shape=[jax.ShapeDtypeStruct((half, wide), kind) for kind in (BF, F32)],
        in_specs=[pl.BlockSpec(memory_space=pltpu.SMEM), vmem, weights, weights],
        out_specs=[result, result],
        cost_estimate=pl.CostEstimate(
            flops=8 * half * depth * wide, bytes_accessed=9 << 20, transcendentals=0
        ),
        name="both_mm",
    )(at, x, own, other)


def near_kernel(at, x, own, other, part, rest, whole):
    ci, zp, xi = at[0], at[1], at[3]
    height = own.shape[0] // 4
    half = x.shape[1]
    for ref, core in ((own, ci), (other, 1 - ci)):
        for k in range(4):
            b = ((xi + 4 - k) & 3) * 2 + core
            to = pl.ds(pl.multiple_of(b * height, 16), height)
            whole[to] = ref[k * height : (k + 1) * height]
    part[...] = dot(x[...], whole[pl.ds(pl.multiple_of(zp * half, 16), half)])
    rest[...] = whole[pl.ds(pl.multiple_of((1 - zp) * half, 16), half)]


def far_kernel(x, part, rest, out):
    rows = x.shape[0]
    total = (part[...] + dot(x[...], rest[...])).astype(BF)
    for zh in range(2):
        for y in range(4):
            n = (zh * 4 + y) * 128
            out[y, zh * rows : (zh + 1) * rows] = total[:, n : n + 128]


def near_part(at, x, own, other):
    rows, half = x.shape
    wide = own.shape[1]
    vmem = pl.BlockSpec(memory_space=pltpu.VMEM)
    return pl.pallas_call(
        near_kernel,
        out_shape=(
            jax.ShapeDtypeStruct((rows, wide), F32),
            jax.ShapeDtypeStruct((half, wide), BF),
        ),
        in_specs=[pl.BlockSpec(memory_space=pltpu.SMEM), vmem, vmem, vmem],
        out_specs=(vmem, vmem),
        scratch_shapes=[pltpu.VMEM((2 * half, wide), BF)],
        cost_estimate=pl.CostEstimate(
            flops=2 * rows * half * wide, bytes_accessed=5 << 20, transcendentals=0
        ),
        name="near_mm",
    )(at, x, own, other)


def down_parts(x, part, rest):
    rows, half = x.shape
    vmem = pl.BlockSpec(memory_space=pltpu.VMEM)
    return pl.pallas_call(
        far_kernel,
        out_shape=jax.ShapeDtypeStruct((4, 2 * rows, 128), BF),
        in_specs=[vmem, vmem, vmem],
        out_specs=vmem,
        cost_estimate=pl.CostEstimate(
            flops=2 * rows * half * 1024, bytes_accessed=3 << 20, transcendentals=0
        ),
        name="far_mm",
    )(x, part, rest)


def exact(value):
    return lax.reduce_precision(value, 8, 7)


def on_device(attn_out, residual, proj_weight, norm_gain, gate_proj, up_proj, down_proj):
    xi, ci, zh = (lax.axis_index(name) for name in ("x", "c", "zh"))
    zq, zp = lax.axis_index("zq"), lax.axis_index("zp")
    at = jnp.stack([ci, zp, 2 * zq + zp, xi]).astype(jnp.int32)
    rows = attn_out.shape[0]
    ffw = gate_proj.shape[1] // 2

    cols = attn_out[None]
    for bit in (4, 2, 1):
        arrived = swap(cols, ZL, bit)
        cols = jnp.concatenate([cols, arrived])

    def columns(which):
        halves = [lax.dynamic_slice_in_dim(w, which * ffw, ffw, 1) for w in (gate_proj, up_proj)]
        return jnp.concatenate(halves, axis=1)

    facing = swap(columns(1 - zp), "zp", 1)
    both = jnp.concatenate([columns(zp), facing])
    both_own, both_other = ring_gathered(both)
    proj_own = from_everyone(proj_weight, "x").reshape(-1, proj_weight.shape[1])
    proj_other = swap(proj_own, "c", 1)
    down_own, down_other = ring_gathered(down_proj)

    high = exact(norm_gain)
    mid = exact(norm_gain - high)
    low = norm_gain - high - mid
    gains = jnp.pad(jnp.stack([high, mid, low]), ((0, 5), (0, 0)))

    part = proj_parts(at, cols, proj_own, proj_other)
    near = exchange(part, "y").astype(F32).sum(axis=0).reshape(2, rows, 128)
    mine = jnp.arange(2)[:, None, None] == zh
    near = jnp.where(mine, near + residual.astype(F32), near).reshape(2 * rows, 128)
    far = swap(jnp.concatenate([near, gains]).astype(BF), "zh", 1).astype(F32)
    stream2 = near + far[: 2 * rows]
    other_gain = far[2 * rows : 2 * rows + 3].sum(axis=0)
    gain2 = jnp.repeat(jnp.stack(in_bits(norm_gain, other_gain, zh)), rows, axis=0)
    squares = jnp.sum((stream2 * stream2).reshape(2, rows, 128), axis=(0, 2))
    scaled2 = (stream2 * gain2).astype(BF)
    squares = jnp.pad(squares, (0, 256 - rows)).reshape(2, 128)
    high = exact(squares)
    tail = jnp.concatenate([high, squares - high, jnp.zeros((4, 128), F32)]).astype(BF)
    model = from_everyone(jnp.concatenate([scaled2, tail]), ("zp", "y"))
    squares = model[:, 2 * rows : 2 * rows + 4].astype(F32).sum(axis=0)
    squares = squares[:2] + squares[2:]

    half, step = rows // 2, rows // 2 - TOP
    bit1, bit2 = zq & 1, zq >> 1
    send, keep = both_parts(at, model, both_own, both_other, half)
    got = swap(send, "zq", 1)
    squares = sum([swap(squares, "zq", k) for k in (1, 2, 3)], squares)
    sums = keep + got.astype(F32)
    sent = lax.dynamic_slice_in_dim(sums, step * (1 - bit2), TOP, 0).astype(BF)
    got = swap(sent, "zq", 2)
    sums = lax.dynamic_slice_in_dim(sums, step * bit2, TOP, 0) + got.astype(F32)
    squares = lax.dynamic_slice_in_dim(squares.reshape(256), half * bit1 + step * bit2, TOP, 0)
    inverse = lax.rsqrt(squares / D + 1e-05)[:, None]
    gate_sum, up_sum = inverse * sums[:, :ffw], inverse * sums[:, ffw:]
    hidden = (jax.nn.silu(gate_sum) * up_sum).astype(BF)
    upper, lower = in_bits(hidden, swap(hidden, "zq", 2), bit2)
    hidden = jnp.concatenate([upper, lower[2 * TOP - half :]])
    hidden = jnp.concatenate(in_bits(hidden, swap(hidden, "zq", 1), bit1))
    hidden, down_other = lax.optimization_barrier((hidden, down_other))
    facing = swap(hidden, "zp", 1)

    part, rest = near_part(at, hidden, down_own, down_other)
    part = down_parts(facing, part, rest)
    near = exchange(part, "y").astype(F32).sum(axis=0).reshape(2, rows, 128)
    far = swap(pick(near, 1 - zh).astype(BF), "zh", 1)
    stream = pick(stream2.reshape(2, rows, 128), zh)
    return (stream + pick(near, zh) + far.astype(F32)).astype(BF)


def solution(mesh):
    z = mesh.shape["gz"] // 4
    split = Mesh(mesh.devices.reshape(4, 2, mesh.shape["gy"] // 2, 2, z, 4), AXES)
    gx, gz = ("x", "c"), ("zh", "y")
    in_specs = (
        P(gx, (*gz, *ZL)),
        P(gx, (*ZL, *gz)),
        P((*gz, *gx), ZL),
        P((*ZL, *gz)),
        P((*ZL, *gx), gz),
        P((*ZL, *gx), gz),
        P((*gz, *gx), ZL),
    )
    return jax.shard_map(
        on_device, mesh=split, in_specs=in_specs, out_specs=P(gx, (*ZL, *gz)), check_vma=False
    )
```

```python
import jax
import jax.numpy as jnp
from jax import lax
from jax.experimental import pallas as pl
from jax.experimental.pallas import tpu as pltpu
from jax.sharding import Mesh
from jax.sharding import PartitionSpec as P


D = 8192
BF = jnp.bfloat16
F32 = jnp.float32
AXES = ("x", "c", "zq", "zp", "zh", "y")
ZL = ("zq", "zp")
TOP = 48


def size_of(axis):
    return lax.axis_size(axis)


def shift(value, axis, step):
    n = size_of(axis)
    return lax.ppermute(value, axis, [(i, (i + step) % n) for i in range(n)])


def swap(value, axis, bit):
    n = size_of(axis)
    return lax.ppermute(value, axis, [(i, i ^ bit) for i in range(n)])


def pick(value, index, dim=0):
    return lax.dynamic_index_in_dim(value, index, dim, keepdims=False)


def exchange(parts, axis):
    return lax.all_to_all(parts, axis, split_axis=0, concat_axis=0, tiled=True)


def from_everyone(value, axis):
    copies = jnp.broadcast_to(value, (size_of(axis), *value.shape))
    return exchange(copies, axis)


def in_bits(own, other, bit):
    first = jnp.where(bit == 0, own, other)
    second = jnp.where(bit == 0, other, own)
    return first, second


def stack_kernel(*refs):
    *ins, out = refs
    height = ins[0].shape[0]
    for k, ref in enumerate(ins):
        out[k * height : (k + 1) * height] = ref[...]


def stacked(parts):
    height, width = parts[0].shape
    vmem = pl.BlockSpec(memory_space=pltpu.VMEM)
    return pl.pallas_call(
        stack_kernel,
        out_shape=jax.ShapeDtypeStruct((len(parts) * height, width), BF),
        in_specs=[vmem] * len(parts),
        out_specs=vmem,
        name="stack",
    )(*parts)


def ring_gathered(w):
    ring = [1, 2, -1]
    shards = [w] + [shift(w, "x", k) for k in ring]
    own = stacked(shards)
    return own, swap(own, "c", 1)


def dot(a, b):
    return jnp.dot(a, b, preferred_element_type=F32)


def proj_kernel(at, first, second, third, fourth, own, other, out, x):
    x[0], x[1], x[2:4], x[4:8] = first[0], second[0], third[...], fourth[...]
    ci, zl = at[0], at[2]
    rows = x.shape[1]

    def blocks(core):
        offs = [(2 * k + core) ^ zl for k in range(4)]
        return [x[((off >> 2) & 1) | (off & 2) | ((off & 1) << 2)] for off in offs]

    mine = jnp.concatenate(blocks(ci), axis=1)
    theirs = jnp.concatenate(blocks(1 - ci), axis=1)
    part = (dot(mine, own[...]) + dot(theirs, other[...])).astype(BF)
    for zh in range(2):
        for y in range(4):
            n = (zh * 4 + y) * 128
            out[y, zh * rows : (zh + 1) * rows] = part[:, n : n + 128]


def proj_parts(at, pieces, own, other):
    rows = pieces[0].shape[1]
    vmem = pl.BlockSpec(memory_space=pltpu.VMEM)
    return pl.pallas_call(
        proj_kernel,
        out_shape=jax.ShapeDtypeStruct((4, 2 * rows, 128), BF),
        in_specs=[pl.BlockSpec(memory_space=pltpu.SMEM)] + [vmem] * 6,
        out_specs=vmem,
        scratch_shapes=[pltpu.VMEM((8, rows, 128), BF)],
        cost_estimate=pl.CostEstimate(
            flops=2 * rows * 1024 * 1024, bytes_accessed=3 << 20, transcendentals=0
        ),
        name="proj_mm",
    )(at, *pieces, own, other)


def both_kernel(at, x, own, other, late_own, late_other, send, keep):
    ci, zp, bit, xi = at[0], at[1], (at[2] >> 1) & 1, at[3]
    rows = (x.shape[1] - 8) // 2

    def blocks(core, steps):
        parts = []
        for k in steps:
            place = (xi + 4 - k) & 3
            row = pl.multiple_of((place >> 1) * rows, 16)
            for turn in range(2):
                at_block = (zp ^ turn) * 4 + (place & 1) * 2 + core
                parts.append(x[at_block, pl.ds(row, rows)])
        return jnp.concatenate(parts, axis=1)

    part = dot(blocks(ci, (0, 2)), own[...]) + dot(blocks(1 - ci, (0, 2)), other[...])
    part += dot(blocks(ci, (1, 3)), late_own[...])
    part += dot(blocks(1 - ci, (1, 3)), late_other[...])
    upper, lower = part[: rows // 2], part[rows // 2 :]
    tile, wide = own.shape[1], send.shape[1] - 128
    cols = pl.ds(pl.multiple_of(pl.program_id(0) * tile, 128), tile)
    send[:, cols] = jnp.where(bit == 0, lower, upper).astype(BF)
    keep[:, cols] = jnp.where(bit == 0, upper, lower)

    @pl.when(pl.program_id(0) == 0)
    def _():
        squares = sum(x[k, pl.ds(2 * rows, 4)].astype(F32) for k in range(8))
        squares = jnp.concatenate([squares[k : k + 1] + squares[k + 2 : k + 3] for k in (0, 1)], 1)
        lane = lax.broadcasted_iota(jnp.int32, (rows // 2, 256), 1)
        row = lax.broadcasted_iota(jnp.int32, (rows // 2, 256), 0)

        def total(half):
            own_lane = jnp.where(lane == row + half * (rows // 2), squares, 0.0)
            return jnp.sum(own_lane, axis=1, keepdims=True)

        send[:, wide:] = in_lanes(total(1 - bit)).astype(BF)
        keep[:, wide:] = in_lanes(total(bit))


def in_lanes(total):
    high = total.astype(BF).astype(F32)
    lane = lax.broadcasted_iota(jnp.int32, (total.shape[0], 128), 1)
    return jnp.where(lane == 0, high, jnp.where(lane == 1, total - high, 0.0))


def both_parts(at, x, weights_of, half):
    depth, wide = weights_of[0].shape
    vmem = pl.BlockSpec(memory_space=pltpu.VMEM)
    weights = pl.BlockSpec((depth, wide // 2), lambda n: (0, n))
    return pl.pallas_call(
        both_kernel,
        grid=(2,),
        out_shape=[jax.ShapeDtypeStruct((half, wide + 128), kind) for kind in (BF, F32)],
        in_specs=[pl.BlockSpec(memory_space=pltpu.SMEM), vmem] + [weights] * 4,
        out_specs=[vmem, vmem],
        cost_estimate=pl.CostEstimate(
            flops=16 * half * depth * wide, bytes_accessed=9 << 20, transcendentals=0
        ),
        name="both_mm",
    )(at, x, *weights_of)


def middle_kernel(at, keep, got, send, rest):
    bit = (at[2] >> 2) & 1
    wide = send.shape[1] - 128
    total = keep[...] + got[...].astype(F32)
    upper, lower = total[:TOP], total[total.shape[0] - TOP :]
    rest[...] = jnp.where(bit == 0, upper, lower)
    sent = jnp.where(bit == 0, lower, upper)
    send[:, :wide] = sent[:, :wide].astype(BF)
    send[:, wide:] = in_lanes(sent[:, wide : wide + 1] + sent[:, wide + 1 : wide + 2]).astype(BF)


def middle(at, keep, got):
    vmem = pl.BlockSpec(memory_space=pltpu.VMEM)
    return pl.pallas_call(
        middle_kernel,
        out_shape=[jax.ShapeDtypeStruct((TOP, keep.shape[1]), kind) for kind in (BF, F32)],
        in_specs=[pl.BlockSpec(memory_space=pltpu.SMEM), vmem, vmem],
        out_specs=[vmem, vmem],
        name="middle",
    )(at, keep, got)


def near_kernel(at, x, own, other, part, rest, whole):
    ci, zp, xi = at[0], at[1], at[3]
    height = own.shape[0] // 4
    half = x.shape[1]
    for ref, core in ((own, ci), (other, 1 - ci)):
        for k in range(4):
            b = ((xi + 4 - k) & 3) * 2 + core
            to = pl.ds(pl.multiple_of(b * height, 16), height)
            whole[to] = ref[k * height : (k + 1) * height]
    part[...] = dot(x[...], whole[pl.ds(pl.multiple_of(zp * half, 16), half)])
    rest[...] = whole[pl.ds(pl.multiple_of((1 - zp) * half, 16), half)]


def far_kernel(x, part, rest, out):
    rows = x.shape[0]
    total = (part[...] + dot(x[...], rest[...])).astype(BF)
    for zh in range(2):
        for y in range(4):
            n = (zh * 4 + y) * 128
            out[y, zh * rows : (zh + 1) * rows] = total[:, n : n + 128]


def near_part(at, x, own, other):
    rows, half = x.shape
    wide = own.shape[1]
    vmem = pl.BlockSpec(memory_space=pltpu.VMEM)
    return pl.pallas_call(
        near_kernel,
        out_shape=(
            jax.ShapeDtypeStruct((rows, wide), F32),
            jax.ShapeDtypeStruct((half, wide), BF),
        ),
        in_specs=[pl.BlockSpec(memory_space=pltpu.SMEM), vmem, vmem, vmem],
        out_specs=(vmem, vmem),
        scratch_shapes=[pltpu.VMEM((2 * half, wide), BF)],
        cost_estimate=pl.CostEstimate(
            flops=2 * rows * half * wide, bytes_accessed=5 << 20, transcendentals=0
        ),
        name="near_mm",
    )(at, x, own, other)


def down_parts(x, part, rest):
    rows, half = x.shape
    vmem = pl.BlockSpec(memory_space=pltpu.VMEM)
    return pl.pallas_call(
        far_kernel,
        out_shape=jax.ShapeDtypeStruct((4, 2 * rows, 128), BF),
        in_specs=[vmem, vmem, vmem],
        out_specs=vmem,
        cost_estimate=pl.CostEstimate(
            flops=2 * rows * half * 1024, bytes_accessed=3 << 20, transcendentals=0
        ),
        name="far_mm",
    )(x, part, rest)


def exact(value):
    return lax.reduce_precision(value, 8, 7)


def on_device(attn_out, residual, proj_weight, norm_gain, gate_proj, up_proj, down_proj):
    xi, ci, zh = (lax.axis_index(name) for name in ("x", "c", "zh"))
    zq, zp = lax.axis_index("zq"), lax.axis_index("zp")
    at = jnp.stack([ci, zp, 2 * zq + zp, xi]).astype(jnp.int32)
    rows = attn_out.shape[0]
    ffw = gate_proj.shape[1] // 2

    cols = attn_out[None]
    pieces = [cols]
    for bit in (4, 2, 1):
        pieces.append(swap(cols, ZL, bit))
        cols = jnp.concatenate(pieces)

    def columns(which):
        halves = [lax.dynamic_slice_in_dim(w, which * ffw, ffw, 1) for w in (gate_proj, up_proj)]
        return jnp.concatenate(halves, axis=1)

    facing = swap(columns(1 - zp), "zp", 1)
    both = jnp.concatenate([columns(zp), facing])
    weights_of = []
    two_hops = shift(both, "x", 2)
    one_hop = [shift(both, "x", 1), shift(both, "x", -1)]
    for shards in ([both, two_hops], one_hop):
        weights_of.append(stacked(shards))
        weights_of.append(swap(weights_of[-1], "c", 1))
    proj_own = from_everyone(proj_weight, "x").reshape(-1, proj_weight.shape[1])
    proj_other = swap(proj_own, "c", 1)
    down_own, down_other = ring_gathered(down_proj)

    high = exact(norm_gain)
    mid = exact(norm_gain - high)
    low = norm_gain - high - mid
    gains = jnp.pad(jnp.stack([high, mid, low]), ((0, 5), (0, 0)))

    part = proj_parts(at, pieces, proj_own, proj_other)
    part, residual = lax.optimization_barrier((part, residual))
    near = exchange(part, "y").astype(F32).sum(axis=0).reshape(2, rows, 128)
    mine = jnp.arange(2)[:, None, None] == zh
    near = jnp.where(mine, near + residual.astype(F32), near).reshape(2 * rows, 128)
    far = swap(jnp.concatenate([near, gains]).astype(BF), "zh", 1).astype(F32)
    stream2 = near + far[: 2 * rows]
    other_gain = far[2 * rows : 2 * rows + 3].sum(axis=0)
    gain2 = jnp.repeat(jnp.stack(in_bits(norm_gain, other_gain, zh)), rows, axis=0)
    squares = jnp.sum((stream2 * stream2).reshape(2, rows, 128), axis=(0, 2))
    scaled2 = (stream2 * gain2).astype(BF)
    squares = jnp.pad(squares, (0, 256 - rows)).reshape(2, 128)
    high = exact(squares)
    tail = jnp.concatenate([high, squares - high, jnp.zeros((4, 128), F32)]).astype(BF)
    model = from_everyone(jnp.concatenate([scaled2, tail]), ("zp", "y"))
    half = rows // 2
    bit1, bit2 = zq & 1, zq >> 1
    send, keep = both_parts(at, model, weights_of, half)
    send, rest = middle(at, keep, swap(send, "zq", 1))
    sums = rest + swap(send, "zq", 2).astype(F32)
    squares = sums[:, 2 * ffw] + sums[:, 2 * ffw + 1]
    inverse = lax.rsqrt(squares / D + 1e-05)[:, None]
    gate_sum, up_sum = inverse * sums[:, :ffw], inverse * sums[:, ffw : 2 * ffw]
    hidden = (jax.nn.silu(gate_sum) * up_sum).astype(BF)
    upper, lower = in_bits(hidden, swap(hidden, "zq", 2), bit2)
    hidden = jnp.concatenate([upper, lower[2 * TOP - half :]])
    hidden = jnp.concatenate(in_bits(hidden, swap(hidden, "zq", 1), bit1))
    hidden, down_other = lax.optimization_barrier((hidden, down_other))
    facing = swap(hidden, "zp", 1)

    part, rest = near_part(at, hidden, down_own, down_other)
    part = down_parts(facing, part, rest)
    near = exchange(part, "y").astype(F32).sum(axis=0).reshape(2, rows, 128)
    far = swap(pick(near, 1 - zh).astype(BF), "zh", 1)
    stream = pick(stream2.reshape(2, rows, 128), zh)
    return (stream + pick(near, zh) + far.astype(F32)).astype(BF)


def solution(mesh):
    z = mesh.shape["gz"] // 4
    split = Mesh(mesh.devices.reshape(4, 2, mesh.shape["gy"] // 2, 2, z, 4), AXES)
    gx, gz = ("x", "c"), ("zh", "y")
    in_specs = (
        P(gx, (*gz, *ZL)),
        P(gx, (*ZL, *gz)),
        P((*gz, *gx), ZL),
        P((*ZL, *gz)),
        P((*ZL, *gx), gz),
        P((*ZL, *gx), gz),
        P((*gz, *gx), ZL),
    )
    return jax.shard_map(
        on_device, mesh=split, in_specs=in_specs, out_specs=P(gx, (*ZL, *gz)), check_vma=False
    )
```

```python
import jax
import jax.numpy as jnp
from jax import lax
from jax.experimental import pallas as pl
from jax.experimental.pallas import tpu as pltpu
from jax.sharding import Mesh
from jax.sharding import PartitionSpec as P


D = 8192
BF = jnp.bfloat16
F32 = jnp.float32
AXES = ("x", "c", "zq", "zp", "zh", "y")
ZL = ("zq", "zp")
TOP = 48


def size_of(axis):
    return lax.axis_size(axis)


def shift(value, axis, step):
    n = size_of(axis)
    return lax.ppermute(value, axis, [(i, (i + step) % n) for i in range(n)])


def swap(value, axis, bit):
    n = size_of(axis)
    return lax.ppermute(value, axis, [(i, i ^ bit) for i in range(n)])


def pick(value, index, dim=0):
    return lax.dynamic_index_in_dim(value, index, dim, keepdims=False)


def exchange(parts, axis):
    return lax.all_to_all(parts, axis, split_axis=0, concat_axis=0, tiled=True)


def from_everyone(value, axis):
    copies = jnp.broadcast_to(value, (size_of(axis), *value.shape))
    return exchange(copies, axis)


def in_bits(own, other, bit):
    first = jnp.where(bit == 0, own, other)
    second = jnp.where(bit == 0, other, own)
    return first, second


def stack_kernel(*refs):
    *ins, out = refs
    height = ins[0].shape[0]
    for k, ref in enumerate(ins):
        out[k * height : (k + 1) * height] = ref[...]


def stacked(parts):
    height, width = parts[0].shape
    vmem = pl.BlockSpec(memory_space=pltpu.VMEM)
    return pl.pallas_call(
        stack_kernel,
        out_shape=jax.ShapeDtypeStruct((len(parts) * height, width), BF),
        in_specs=[vmem] * len(parts),
        out_specs=vmem,
        name="stack",
    )(*parts)


def ring_gathered(w):
    ring = [1, 2, -1]
    shards = [w] + [shift(w, "x", k) for k in ring]
    own = stacked(shards)
    return own, swap(own, "c", 1)


def dot(a, b):
    return jnp.dot(a, b, preferred_element_type=F32)


def proj_kernel(at, first, second, third, fourth, own, other, out, x):
    x[0], x[1], x[2:4], x[4:8] = first[0], second[0], third[...], fourth[...]
    ci, zl = at[0], at[2]
    rows = x.shape[1]

    def blocks(core):
        offs = [(2 * k + core) ^ zl for k in range(4)]
        return [x[((off >> 2) & 1) | (off & 2) | ((off & 1) << 2)] for off in offs]

    mine = jnp.concatenate(blocks(ci), axis=1)
    theirs = jnp.concatenate(blocks(1 - ci), axis=1)
    part = (dot(mine, own[...]) + dot(theirs, other[...])).astype(BF)
    for zh in range(2):
        for y in range(4):
            n = (zh * 4 + y) * 128
            out[y, zh * rows : (zh + 1) * rows] = part[:, n : n + 128]


def proj_parts(at, pieces, own, other):
    rows = pieces[0].shape[1]
    vmem = pl.BlockSpec(memory_space=pltpu.VMEM)
    return pl.pallas_call(
        proj_kernel,
        out_shape=jax.ShapeDtypeStruct((4, 2 * rows, 128), BF),
        in_specs=[pl.BlockSpec(memory_space=pltpu.SMEM)] + [vmem] * 6,
        out_specs=vmem,
        scratch_shapes=[pltpu.VMEM((8, rows, 128), BF)],
        cost_estimate=pl.CostEstimate(
            flops=2 * rows * 1024 * 1024, bytes_accessed=3 << 20, transcendentals=0
        ),
        name="proj_mm",
    )(at, *pieces, own, other)


def both_kernel(at, x, own, other, send, keep):
    ci, zp, bit, xi = at[0], at[1], (at[2] >> 1) & 1, at[3]
    rows = (x.shape[1] - 8) // 2

    def blocks(core):
        parts = []
        for k in range(4):
            place = (xi + 4 - k) & 3
            row = pl.multiple_of((place >> 1) * rows, 16)
            for turn in range(2):
                at_block = (zp ^ turn) * 4 + (place & 1) * 2 + core
                parts.append(x[at_block, pl.ds(row, rows)])
        return jnp.concatenate(parts, axis=1)

    part = dot(blocks(ci), own[...]) + dot(blocks(1 - ci), other[...])
    upper, lower = part[: rows // 2], part[rows // 2 :]
    tile, wide = own.shape[1], send.shape[1] - 128
    cols = pl.ds(pl.multiple_of(pl.program_id(0) * tile, 128), tile)
    send[:, cols] = jnp.where(bit == 0, lower, upper).astype(BF)
    keep[:, cols] = jnp.where(bit == 0, upper, lower)

    @pl.when(pl.program_id(0) == 0)
    def _():
        squares = sum(x[k, pl.ds(2 * rows, 4)].astype(F32) for k in range(8))
        squares = jnp.concatenate([squares[k : k + 1] + squares[k + 2 : k + 3] for k in (0, 1)], 1)
        lane = lax.broadcasted_iota(jnp.int32, (rows // 2, 256), 1)
        row = lax.broadcasted_iota(jnp.int32, (rows // 2, 256), 0)

        def total(half):
            own_lane = jnp.where(lane == row + half * (rows // 2), squares, 0.0)
            return jnp.sum(own_lane, axis=1, keepdims=True)

        send[:, wide:] = in_lanes(total(1 - bit)).astype(BF)
        keep[:, wide:] = in_lanes(total(bit))


def in_lanes(total):
    high = total.astype(BF).astype(F32)
    lane = lax.broadcasted_iota(jnp.int32, (total.shape[0], 128), 1)
    return jnp.where(lane == 0, high, jnp.where(lane == 1, total - high, 0.0))


def both_parts(at, x, own, other, half):
    depth, wide = own.shape
    vmem = pl.BlockSpec(memory_space=pltpu.VMEM)
    weights = pl.BlockSpec((depth, wide // 2), lambda n: (0, n))
    return pl.pallas_call(
        both_kernel,
        grid=(2,),
        out_shape=[jax.ShapeDtypeStruct((half, wide + 128), kind) for kind in (BF, F32)],
        in_specs=[pl.BlockSpec(memory_space=pltpu.SMEM), vmem, weights, weights],
        out_specs=[vmem, vmem],
        cost_estimate=pl.CostEstimate(
            flops=8 * half * depth * wide, bytes_accessed=9 << 20, transcendentals=0
        ),
        name="both_mm",
    )(at, x, own, other)


def middle_kernel(at, keep, got, send, rest):
    bit = (at[2] >> 2) & 1
    wide = send.shape[1] - 128
    total = keep[...] + got[...].astype(F32)
    upper, lower = total[:TOP], total[total.shape[0] - TOP :]
    rest[...] = jnp.where(bit == 0, upper, lower)
    sent = jnp.where(bit == 0, lower, upper)
    send[:, :wide] = sent[:, :wide].astype(BF)
    send[:, wide:] = in_lanes(sent[:, wide : wide + 1] + sent[:, wide + 1 : wide + 2]).astype(BF)


def middle(at, keep, got):
    vmem = pl.BlockSpec(memory_space=pltpu.VMEM)
    return pl.pallas_call(
        middle_kernel,
        out_shape=[jax.ShapeDtypeStruct((TOP, keep.shape[1]), kind) for kind in (BF, F32)],
        in_specs=[pl.BlockSpec(memory_space=pltpu.SMEM), vmem, vmem],
        out_specs=[vmem, vmem],
        name="middle",
    )(at, keep, got)


def near_kernel(at, x, own, other, part, rest, whole):
    ci, zp, xi = at[0], at[1], at[3]
    height = own.shape[0] // 4
    half = x.shape[1]
    for ref, core in ((own, ci), (other, 1 - ci)):
        for k in range(4):
            b = ((xi + 4 - k) & 3) * 2 + core
            to = pl.ds(pl.multiple_of(b * height, 16), height)
            whole[to] = ref[k * height : (k + 1) * height]
    part[...] = dot(x[...], whole[pl.ds(pl.multiple_of(zp * half, 16), half)])
    rest[...] = whole[pl.ds(pl.multiple_of((1 - zp) * half, 16), half)]


def far_kernel(x, part, rest, out):
    rows = x.shape[0]
    total = (part[...] + dot(x[...], rest[...])).astype(BF)
    for zh in range(2):
        for y in range(4):
            n = (zh * 4 + y) * 128
            out[y, zh * rows : (zh + 1) * rows] = total[:, n : n + 128]


def near_part(at, x, own, other):
    rows, half = x.shape
    wide = own.shape[1]
    vmem = pl.BlockSpec(memory_space=pltpu.VMEM)
    return pl.pallas_call(
        near_kernel,
        out_shape=(
            jax.ShapeDtypeStruct((rows, wide), F32),
            jax.ShapeDtypeStruct((half, wide), BF),
        ),
        in_specs=[pl.BlockSpec(memory_space=pltpu.SMEM), vmem, vmem, vmem],
        out_specs=(vmem, vmem),
        scratch_shapes=[pltpu.VMEM((2 * half, wide), BF)],
        cost_estimate=pl.CostEstimate(
            flops=2 * rows * half * wide, bytes_accessed=5 << 20, transcendentals=0
        ),
        name="near_mm",
    )(at, x, own, other)


def down_parts(x, part, rest):
    rows, half = x.shape
    vmem = pl.BlockSpec(memory_space=pltpu.VMEM)
    return pl.pallas_call(
        far_kernel,
        out_shape=jax.ShapeDtypeStruct((4, 2 * rows, 128), BF),
        in_specs=[vmem, vmem, vmem],
        out_specs=vmem,
        cost_estimate=pl.CostEstimate(
            flops=2 * rows * half * 1024, bytes_accessed=3 << 20, transcendentals=0
        ),
        name="far_mm",
    )(x, part, rest)


def exact(value):
    return lax.reduce_precision(value, 8, 7)


def on_device(attn_out, residual, proj_weight, norm_gain, gate_proj, up_proj, down_proj):
    xi, ci, zh = (lax.axis_index(name) for name in ("x", "c", "zh"))
    zq, zp = lax.axis_index("zq"), lax.axis_index("zp")
    at = jnp.stack([ci, zp, 2 * zq + zp, xi]).astype(jnp.int32)
    rows = attn_out.shape[0]
    ffw = gate_proj.shape[1] // 2

    cols = attn_out[None]
    pieces = [cols]
    for bit in (4, 2, 1):
        pieces.append(swap(cols, ZL, bit))
        cols = jnp.concatenate(pieces)

    def columns(which):
        halves = [lax.dynamic_slice_in_dim(w, which * ffw, ffw, 1) for w in (gate_proj, up_proj)]
        return jnp.concatenate(halves, axis=1)

    facing = swap(columns(1 - zp), "zp", 1)
    both = jnp.concatenate([columns(zp), facing])
    both_own, both_other = ring_gathered(both)
    proj_own = from_everyone(proj_weight, "x").reshape(-1, proj_weight.shape[1])
    proj_other = swap(proj_own, "c", 1)
    down_own, down_other = ring_gathered(down_proj)

    high = exact(norm_gain)
    mid = exact(norm_gain - high)
    low = norm_gain - high - mid
    gains = jnp.pad(jnp.stack([high, mid, low]), ((0, 5), (0, 0)))

    part = proj_parts(at, pieces, proj_own, proj_other)
    part, residual = lax.optimization_barrier((part, residual))
    near = exchange(part, "y").astype(F32).sum(axis=0).reshape(2, rows, 128)
    mine = jnp.arange(2)[:, None, None] == zh
    near = jnp.where(mine, near + residual.astype(F32), near).reshape(2 * rows, 128)
    far = swap(jnp.concatenate([near, gains]).astype(BF), "zh", 1).astype(F32)
    stream2 = near + far[: 2 * rows]
    other_gain = far[2 * rows : 2 * rows + 3].sum(axis=0)
    gain2 = jnp.repeat(jnp.stack(in_bits(norm_gain, other_gain, zh)), rows, axis=0)
    squares = jnp.sum((stream2 * stream2).reshape(2, rows, 128), axis=(0, 2))
    scaled2 = (stream2 * gain2).astype(BF)
    squares = jnp.pad(squares, (0, 256 - rows)).reshape(2, 128)
    high = exact(squares)
    tail = jnp.concatenate([high, squares - high, jnp.zeros((4, 128), F32)]).astype(BF)
    model = from_everyone(jnp.concatenate([scaled2, tail]), ("zp", "y"))
    half = rows // 2
    bit1, bit2 = zq & 1, zq >> 1
    send, keep = both_parts(at, model, both_own, both_other, half)
    send, rest = middle(at, keep, swap(send, "zq", 1))
    sums = rest + swap(send, "zq", 2).astype(F32)
    squares = sums[:, 2 * ffw] + sums[:, 2 * ffw + 1]
    inverse = lax.rsqrt(squares / D + 1e-05)[:, None]
    gate_sum, up_sum = inverse * sums[:, :ffw], inverse * sums[:, ffw : 2 * ffw]
    hidden = (jax.nn.silu(gate_sum) * up_sum).astype(BF)
    upper, lower = in_bits(hidden, swap(hidden, "zq", 2), bit2)
    hidden = jnp.concatenate([upper, lower[2 * TOP - half :]])
    hidden = jnp.concatenate(in_bits(hidden, swap(hidden, "zq", 1), bit1))
    hidden, down_other = lax.optimization_barrier((hidden, down_other))
    facing = swap(hidden, "zp", 1)

    part, rest = near_part(at, hidden, down_own, down_other)
    part = down_parts(facing, part, rest)
    near = exchange(part, "y").astype(F32).sum(axis=0).reshape(2, rows, 128)
    far = swap(pick(near, 1 - zh).astype(BF), "zh", 1)
    stream = pick(stream2.reshape(2, rows, 128), zh)
    return (stream + pick(near, zh) + far.astype(F32)).astype(BF)


def solution(mesh):
    z = mesh.shape["gz"] // 4
    split = Mesh(mesh.devices.reshape(4, 2, mesh.shape["gy"] // 2, 2, z, 4), AXES)
    gx, gz = ("x", "c"), ("zh", "y")
    in_specs = (
        P(gx, (*gz, *ZL)),
        P(gx, (*ZL, *gz)),
        P((*gz, *gx), ZL),
        P((*ZL, *gz)),
        P((*ZL, *gx), gz),
        P((*ZL, *gx), gz),
        P((*gz, *gx), ZL),
    )
    return jax.shard_map(
        on_device, mesh=split, in_specs=in_specs, out_specs=P(gx, (*ZL, *gz)), check_vma=False
    )
```

```python
import jax
import jax.numpy as jnp
from jax import lax
from jax.experimental import pallas as pl
from jax.experimental.pallas import tpu as pltpu
from jax.sharding import Mesh
from jax.sharding import PartitionSpec as P


D = 8192
BF = jnp.bfloat16
F32 = jnp.float32
AXES = ("x", "c", "zq", "zp", "zh", "y")
ZL = ("zq", "zp")
TOP = 48


def size_of(axis):
    return lax.axis_size(axis)


def shift(value, axis, step):
    n = size_of(axis)
    return lax.ppermute(value, axis, [(i, (i + step) % n) for i in range(n)])


def swap(value, axis, bit):
    n = size_of(axis)
    return lax.ppermute(value, axis, [(i, i ^ bit) for i in range(n)])


def pick(value, index, dim=0):
    return lax.dynamic_index_in_dim(value, index, dim, keepdims=False)


def exchange(parts, axis):
    return lax.all_to_all(parts, axis, split_axis=0, concat_axis=0, tiled=True)


def from_everyone(value, axis):
    copies = jnp.broadcast_to(value, (size_of(axis), *value.shape))
    return exchange(copies, axis)


def in_bits(own, other, bit):
    first = jnp.where(bit == 0, own, other)
    second = jnp.where(bit == 0, other, own)
    return first, second


def stack_kernel(*refs):
    *ins, out = refs
    height = ins[0].shape[0]
    for k, ref in enumerate(ins):
        out[k * height : (k + 1) * height] = ref[...]


def stacked(parts):
    height, width = parts[0].shape
    vmem = pl.BlockSpec(memory_space=pltpu.VMEM)
    return pl.pallas_call(
        stack_kernel,
        out_shape=jax.ShapeDtypeStruct((len(parts) * height, width), BF),
        in_specs=[vmem] * len(parts),
        out_specs=vmem,
        name="stack",
    )(*parts)


def ring_gathered(w):
    ring = [1, 2, -1]
    shards = [w] + [shift(w, "x", k) for k in ring]
    own = stacked(shards)
    return own, swap(own, "c", 1)


def dot(a, b):
    return jnp.dot(a, b, preferred_element_type=F32)


def proj_kernel(at, first, second, third, fourth, own, other, out, x):
    x[0], x[1], x[2:4], x[4:8] = first[0], second[0], third[...], fourth[...]
    ci, zl = at[0], at[2]
    rows = x.shape[1]

    def blocks(core):
        offs = [(2 * k + core) ^ zl for k in range(4)]
        return [x[((off >> 2) & 1) | (off & 2) | ((off & 1) << 2)] for off in offs]

    mine = jnp.concatenate(blocks(ci), axis=1)
    theirs = jnp.concatenate(blocks(1 - ci), axis=1)
    part = (dot(mine, own[...]) + dot(theirs, other[...])).astype(BF)
    for zh in range(2):
        for y in range(4):
            n = (zh * 4 + y) * 128
            out[y, zh * rows : (zh + 1) * rows] = part[:, n : n + 128]


def proj_parts(at, pieces, own, other):
    rows = pieces[0].shape[1]
    vmem = pl.BlockSpec(memory_space=pltpu.VMEM)
    return pl.pallas_call(
        proj_kernel,
        out_shape=jax.ShapeDtypeStruct((4, 2 * rows, 128), BF),
        in_specs=[pl.BlockSpec(memory_space=pltpu.SMEM)] + [vmem] * 6,
        out_specs=vmem,
        scratch_shapes=[pltpu.VMEM((8, rows, 128), BF)],
        cost_estimate=pl.CostEstimate(
            flops=2 * rows * 1024 * 1024, bytes_accessed=3 << 20, transcendentals=0
        ),
        name="proj_mm",
    )(at, *pieces, own, other)


def both_kernel(at, x, own, other, send, keep):
    ci, zp, bit, xi = at[0], at[1], (at[2] >> 1) & 1, at[3]
    rows = (x.shape[1] - 8) // 2

    def blocks(core):
        parts = []
        for k in range(4):
            place = (xi + 4 - k) & 3
            row = pl.multiple_of((place >> 1) * rows, 16)
            for turn in range(2):
                at_block = (zp ^ turn) * 4 + (place & 1) * 2 + core
                parts.append(x[at_block, pl.ds(row, rows)])
        return jnp.concatenate(parts, axis=1)

    part = dot(blocks(ci), own[...]) + dot(blocks(1 - ci), other[...])
    upper, lower = part[: rows // 2], part[rows // 2 :]
    send[...] = jnp.where(bit == 0, lower, upper).astype(BF)
    keep[...] = jnp.where(bit == 0, upper, lower)


def both_parts(at, x, own, other, half):
    depth, wide = own.shape
    tile = wide // 2
    vmem = pl.BlockSpec(memory_space=pltpu.VMEM)
    weights = pl.BlockSpec((depth, tile), lambda n: (0, n))
    result = pl.BlockSpec((half, tile), lambda n: (0, n))
    return pl.pallas_call(
        both_kernel,
        grid=(2,),
        out_shape=[jax.ShapeDtypeStruct((half, wide), kind) for kind in (BF, F32)],
        in_specs=[pl.BlockSpec(memory_space=pltpu.SMEM), vmem, weights, weights],
        out_specs=[result, result],
        cost_estimate=pl.CostEstimate(
            flops=8 * half * depth * wide, bytes_accessed=9 << 20, transcendentals=0
        ),
        name="both_mm",
    )(at, x, own, other)


def near_kernel(at, x, own, other, part, rest, whole):
    ci, zp, xi = at[0], at[1], at[3]
    height = own.shape[0] // 4
    half = x.shape[1]
    for ref, core in ((own, ci), (other, 1 - ci)):
        for k in range(4):
            b = ((xi + 4 - k) & 3) * 2 + core
            to = pl.ds(pl.multiple_of(b * height, 16), height)
            whole[to] = ref[k * height : (k + 1) * height]
    part[...] = dot(x[...], whole[pl.ds(pl.multiple_of(zp * half, 16), half)])
    rest[...] = whole[pl.ds(pl.multiple_of((1 - zp) * half, 16), half)]


def far_kernel(x, part, rest, out):
    rows = x.shape[0]
    total = (part[...] + dot(x[...], rest[...])).astype(BF)
    for zh in range(2):
        for y in range(4):
            n = (zh * 4 + y) * 128
            out[y, zh * rows : (zh + 1) * rows] = total[:, n : n + 128]


def near_part(at, x, own, other):
    rows, half = x.shape
    wide = own.shape[1]
    vmem = pl.BlockSpec(memory_space=pltpu.VMEM)
    return pl.pallas_call(
        near_kernel,
        out_shape=(
            jax.ShapeDtypeStruct((rows, wide), F32),
            jax.ShapeDtypeStruct((half, wide), BF),
        ),
        in_specs=[pl.BlockSpec(memory_space=pltpu.SMEM), vmem, vmem, vmem],
        out_specs=(vmem, vmem),
        scratch_shapes=[pltpu.VMEM((2 * half, wide), BF)],
        cost_estimate=pl.CostEstimate(
            flops=2 * rows * half * wide, bytes_accessed=5 << 20, transcendentals=0
        ),
        name="near_mm",
    )(at, x, own, other)


def down_parts(x, part, rest):
    rows, half = x.shape
    vmem = pl.BlockSpec(memory_space=pltpu.VMEM)
    return pl.pallas_call(
        far_kernel,
        out_shape=jax.ShapeDtypeStruct((4, 2 * rows, 128), BF),
        in_specs=[vmem, vmem, vmem],
        out_specs=vmem,
        cost_estimate=pl.CostEstimate(
            flops=2 * rows * half * 1024, bytes_accessed=3 << 20, transcendentals=0
        ),
        name="far_mm",
    )(x, part, rest)


def exact(value):
    return lax.reduce_precision(value, 8, 7)


def on_device(attn_out, residual, proj_weight, norm_gain, gate_proj, up_proj, down_proj):
    xi, ci, zh = (lax.axis_index(name) for name in ("x", "c", "zh"))
    zq, zp = lax.axis_index("zq"), lax.axis_index("zp")
    at = jnp.stack([ci, zp, 2 * zq + zp, xi]).astype(jnp.int32)
    rows = attn_out.shape[0]
    ffw = gate_proj.shape[1] // 2

    cols = attn_out[None]
    pieces = [cols]
    for bit in (4, 2, 1):
        pieces.append(swap(cols, ZL, bit))
        cols = jnp.concatenate(pieces)

    def columns(which):
        halves = [lax.dynamic_slice_in_dim(w, which * ffw, ffw, 1) for w in (gate_proj, up_proj)]
        return jnp.concatenate(halves, axis=1)

    facing = swap(columns(1 - zp), "zp", 1)
    both = jnp.concatenate([columns(zp), facing])
    both_own, both_other = ring_gathered(both)
    proj_own = from_everyone(proj_weight, "x").reshape(-1, proj_weight.shape[1])
    proj_other = swap(proj_own, "c", 1)
    down_own, down_other = ring_gathered(down_proj)

    high = exact(norm_gain)
    mid = exact(norm_gain - high)
    low = norm_gain - high - mid
    gains = jnp.pad(jnp.stack([high, mid, low]), ((0, 5), (0, 0)))

    part = proj_parts(at, pieces, proj_own, proj_other)
    part, residual = lax.optimization_barrier((part, residual))
    near = exchange(part, "y").astype(F32).sum(axis=0).reshape(2, rows, 128)
    mine = jnp.arange(2)[:, None, None] == zh
    near = jnp.where(mine, near + residual.astype(F32), near).reshape(2 * rows, 128)
    far = swap(jnp.concatenate([near, gains]).astype(BF), "zh", 1).astype(F32)
    stream2 = near + far[: 2 * rows]
    other_gain = far[2 * rows : 2 * rows + 3].sum(axis=0)
    gain2 = jnp.repeat(jnp.stack(in_bits(norm_gain, other_gain, zh)), rows, axis=0)
    squares = jnp.sum((stream2 * stream2).reshape(2, rows, 128), axis=(0, 2))
    scaled2 = (stream2 * gain2).astype(BF)
    squares = jnp.pad(squares, (0, 256 - rows)).reshape(2, 128)
    high = exact(squares)
    tail = jnp.concatenate([high, squares - high, jnp.zeros((4, 128), F32)]).astype(BF)
    model = from_everyone(jnp.concatenate([scaled2, tail]), ("zp", "y"))
    squares = model[:, 2 * rows : 2 * rows + 4].astype(F32).sum(axis=0)
    squares = squares[:2] + squares[2:]

    half, step = rows // 2, rows // 2 - TOP
    bit1, bit2 = zq & 1, zq >> 1
    send, keep = both_parts(at, model, both_own, both_other, half)
    got = swap(send, "zq", 1)
    squares = sum([swap(squares, "zq", k) for k in (1, 2, 3)], squares)
    sums = keep + got.astype(F32)
    sent = lax.dynamic_slice_in_dim(sums, step * (1 - bit2), TOP, 0).astype(BF)
    got = swap(sent, "zq", 2)
    sums = lax.dynamic_slice_in_dim(sums, step * bit2, TOP, 0) + got.astype(F32)
    squares = lax.dynamic_slice_in_dim(squares.reshape(256), half * bit1 + step * bit2, TOP, 0)
    inverse = lax.rsqrt(squares / D + 1e-05)[:, None]
    gate_sum, up_sum = inverse * sums[:, :ffw], inverse * sums[:, ffw:]
    hidden = (jax.nn.silu(gate_sum) * up_sum).astype(BF)
    upper, lower = in_bits(hidden, swap(hidden, "zq", 2), bit2)
    hidden = jnp.concatenate([upper, lower[2 * TOP - half :]])
    hidden = jnp.concatenate(in_bits(hidden, swap(hidden, "zq", 1), bit1))
    hidden, down_other = lax.optimization_barrier((hidden, down_other))
    facing = swap(hidden, "zp", 1)

    part, rest = near_part(at, hidden, down_own, down_other)
    part = down_parts(facing, part, rest)
    near = exchange(part, "y").astype(F32).sum(axis=0).reshape(2, rows, 128)
    far = swap(pick(near, 1 - zh).astype(BF), "zh", 1)
    stream = pick(stream2.reshape(2, rows, 128), zh)
    return (stream + pick(near, zh) + far.astype(F32)).astype(BF)


def solution(mesh):
    z = mesh.shape["gz"] // 4
    split = Mesh(mesh.devices.reshape(4, 2, mesh.shape["gy"] // 2, 2, z, 4), AXES)
    gx, gz = ("x", "c"), ("zh", "y")
    in_specs = (
        P(gx, (*gz, *ZL)),
        P(gx, (*ZL, *gz)),
        P((*gz, *gx), ZL),
        P((*ZL, *gz)),
        P((*ZL, *gx), gz),
        P((*ZL, *gx), gz),
        P((*gz, *gx), ZL),
    )
    return jax.shard_map(
        on_device, mesh=split, in_specs=in_specs, out_specs=P(gx, (*ZL, *gz)), check_vma=False
    )
```
